64 devices in a mesh: rep: 4 (over x, y), dp: 16 (over z, core).
Axes of the slice: x: 2, y: 2, z: 8, core: 2. Of those that a mesh axis runs over, the one named last changes fastest.
The devices are a block of a 4x4x8 slice.
Arguments:
- x: bfloat16 [64, 2048, 512], P(('rep', 'dp')), parts along dimension 0
- dy: bfloat16 [64, 2048, 512], P(('rep', 'dp')), parts along dimension 0
- wq: bfloat16 [2, 512, 512], replicated
- wk: bfloat16 [2, 512, 512], replicated
- wv: bfloat16 [2, 512, 512], replicated
- wo: bfloat16 [2, 512, 512], replicated
- w_gate: bfloat16 [2, 512, 2048], replicated
- w_up: bfloat16 [2, 512, 2048], replicated
- w_down: bfloat16 [2, 2048, 512], replicated
- m_wq: float32 [2, 512, 512], P(None, 'dp')
- m_wk: float32 [2, 512, 512], P(None, 'dp')
- m_wv: float32 [2, 512, 512], P(None, 'dp')
- m_wo: float32 [2, 512, 512], P(None, 'dp')
- m_w_gate: float32 [2, 512, 2048], P(None, 'dp')
- m_w_up: float32 [2, 512, 2048], P(None, 'dp')
- m_w_down: float32 [2, 2048, 512], P(None, 'dp')
- v_wq: float32 [2, 512, 512], P(None, 'dp')
- v_wk: float32 [2, 512, 512], P(None, 'dp')
- v_wv: float32 [2, 512, 512], P(None, 'dp')
- v_wo: float32 [2, 512, 512], P(None, 'dp')
- v_w_gate: float32 [2, 512, 2048], P(None, 'dp')
- v_w_up: float32 [2, 512, 2048], P(None, 'dp')
- v_w_down: float32 [2, 2048, 512], P(None, 'dp')
Outputs:
- output 1: bfloat16 [8, 512, 512], P('rep'), parts along dimension 0
- output 2: bfloat16 [8, 512, 512], P('rep'), parts along dimension 0
- output 3: bfloat16 [8, 512, 512], P('rep'), parts along dimension 0
- output 4: bfloat16 [8, 512, 512], P('rep'), parts along dimension 0
- output 5: bfloat16 [8, 512, 2048], P('rep'), parts along dimension 0
- output 6: bfloat16 [8, 512, 2048], P('rep'), parts along dimension 0
- output 7: bfloat16 [8, 2048, 512], P('rep'), parts along dimension 0
- output 8: float32 [8, 512, 512], P('rep', 'dp'), parts along dimension 0
- output 9: float32 [8, 512, 512], P('rep', 'dp'), parts along dimension 0
- output 10: float32 [8, 512, 512], P('rep', 'dp'), parts along dimension 0
- output 11: float32 [8, 512, 512], P('rep', 'dp'), parts along dimension 0
- output 12: float32 [8, 512, 2048], P('rep', 'dp'), parts along dimension 0
- output 13: float32 [8, 512, 2048], P('rep', 'dp'), parts along dimension 0
- output 14: float32 [8, 2048, 512], P('rep', 'dp'), parts along dimension 0
- output 15: float32 [8, 512, 512], P('rep', 'dp'), parts along dimension 0
- output 16: float32 [8, 512, 512], P('rep', 'dp'), parts along dimension 0
- output 17: float32 [8, 512, 512], P('rep', 'dp'), parts along dimension 0
- output 18: float32 [8, 512, 512], P('rep', 'dp'), parts along dimension 0
- output 19: float32 [8, 512, 2048], P('rep', 'dp'), parts along dimension 0
- output 20: float32 [8, 512, 2048], P('rep', 'dp'), parts along dimension 0
- output 21: float32 [8, 2048, 512], P('rep', 'dp'), parts along dimension 0
There are 4 independent parts. The reference program is written for one: setup_inputs(seed, part) draws one part's arguments, and reference() takes and returns one part's arrays. A program takes and returns all parts, laid end to end along the dimension named above; an argument that names none is the same for every part.
All inputs are finite; a program needn't handle non-finite values.
Results may differ from the reference program's by a relative error of at most 0.024.
Values are sent between devices in bfloat16 or wider.
A program may use at most 768 MiB of HBM per device.

```python
import jax
import jax.numpy as jnp
from jax import lax

SEQUENCES = 16
TOKENS = 2048
D = 512
HEADS = 2
KV_HEADS = 2
HEAD = 256
FF = 2048
LAYERS = 2
THETA = 10000
NAMES = ("wq", "wk", "wv", "wo", "w_gate", "w_up", "w_down")
SHAPES = {
    "wq": (LAYERS, D, HEADS * HEAD),
    "wk": (LAYERS, D, KV_HEADS * HEAD),
    "wv": (LAYERS, D, KV_HEADS * HEAD),
    "wo": (LAYERS, HEADS * HEAD, D),
    "w_gate": (LAYERS, D, FF),
    "w_up": (LAYERS, D, FF),
    "w_down": (LAYERS, FF, D),
}


def bump(key, n, height):
    away = (jnp.arange(n, dtype=jnp.int32) - jax.random.randint(key, (), 0, n, jnp.int32)) % n
    return jnp.where(away < n // 8, height, 1.0)


def together(key, own, strength):
    shared = jax.random.normal(key, own.shape[1:], jnp.float32)
    return (own + strength * shared) * lax.rsqrt(1 + strength * strength)


def setup_inputs(seed: int = 0, part: int = 0) -> dict:
    kx, kdy, ka, kb, kz, kf, kh, kl, *keys = jax.random.split(jax.random.key(seed), 8 + 3 * len(NAMES))
    kx, kdy, ka, kb = (jax.random.fold_in(k, part) for k in (kx, kdy, ka, kb))
    kw, km, kv = (keys[i::3] for i in range(3))
    shape = (SEQUENCES, TOKENS, D)
    much_x, much_dy = jax.random.uniform(kz, (2,), jnp.float32, 0.0, 1.0)
    loud = 2.0 ** jax.random.uniform(jax.random.fold_in(kz, 1), (), jnp.float32, -1.0, 2.0)
    layers = 2.0 ** jax.random.uniform(kl, (LAYERS, 1, 1), jnp.float32, -1.0, 1.0)
    times = {"wq": 1.0, "wk": 1.0, "wv": 2.0, "wo": layers, "w_gate": 1.0, "w_up": bump(kh, FF, 4.0), "w_down": layers}
    x = together(ka, jax.random.normal(kx, shape, jnp.float32), much_x) * bump(kf, D, 4.0)
    dy = together(kb, jax.random.normal(kdy, shape, jnp.float32), much_dy)
    drawn = {"x": x.astype(jnp.bfloat16), "dy": (loud * dy * (SEQUENCES * TOKENS) ** -0.5).astype(jnp.bfloat16)}
    for key, name in zip(kw, NAMES, strict=True):
        drawn[name] = (jax.random.normal(key, SHAPES[name], jnp.float32) * SHAPES[name][1] ** -0.5 * times[name]).astype(jnp.bfloat16)
    for key, name in zip(km, NAMES, strict=True):
        drawn[f"m_{name}"] = 0.1 * jax.random.normal(key, SHAPES[name], jnp.float32)
    for key, name in zip(kv, NAMES, strict=True):
        drawn[f"v_{name}"] = loud * loud * jax.random.uniform(key, SHAPES[name], jnp.float32, 0.2, 0.6)
    return drawn


def matmul(a, w):
    return jnp.dot(a, w, preferred_element_type=jnp.float32).astype(jnp.bfloat16)


def normed(h):
    wide = h.astype(jnp.float32)
    scale = lax.rsqrt(jnp.mean(wide**2, -1, keepdims=True) + 1e-6)
    return (wide * scale).astype(jnp.bfloat16)


def turned(t, theta):
    half = t.shape[-1] // 2
    angle = jnp.arange(t.shape[0], dtype=jnp.float32)[:, None] * theta ** (-jnp.arange(half, dtype=jnp.float32) / half)
    cos, sin = jnp.cos(angle)[:, None], jnp.sin(angle)[:, None]
    a, b = t[..., :half].astype(jnp.float32), t[..., half:].astype(jnp.float32)
    return jnp.concatenate([a * cos - b * sin, b * cos + a * sin], -1).astype(jnp.bfloat16)


def seen_by(q, k, v):
    tokens, kv = q.shape[0], k.shape[1]
    q = q.reshape(tokens, kv, -1, q.shape[-1])
    scores = jnp.einsum("tgsd,ugd->gstu", q.astype(jnp.float32), k.astype(jnp.float32)) * q.shape[-1] ** -0.5
    place = jnp.arange(tokens)
    weights = jax.nn.softmax(jnp.where(place[:, None] >= place, scores, -jnp.inf), -1).astype(jnp.bfloat16)
    return jnp.einsum("gstu,ugd->tgsd", weights.astype(jnp.float32), v.astype(jnp.float32)).astype(jnp.bfloat16).reshape(tokens, -1)


def layer(h, w):
    a = normed(h)
    q, k = (turned(matmul(a, w[name]).reshape(h.shape[0], -1, HEAD), THETA) for name in ("wq", "wk"))
    h = h + matmul(seen_by(q, k, matmul(a, w["wv"]).reshape(h.shape[0], -1, HEAD)), w["wo"])
    b = normed(h)
    gate = jnp.dot(b, w["w_gate"], preferred_element_type=jnp.float32)
    up = jnp.dot(b, w["w_up"], preferred_element_type=jnp.float32)
    return h + matmul((jax.nn.silu(gate) * up).astype(jnp.bfloat16), w["w_down"])


def adamw(w, m, v, g):
    m = 0.9 * m + 0.1 * g
    v = 0.95 * v + 0.05 * g * g
    step = m * lax.rsqrt(v + 1e-8) + 0.1 * w
    return (w - 0.02 * step).astype(jnp.bfloat16), m, v


def stack(weights, h):
    return lax.scan(lambda h, w: (layer(h, w), None), h, weights)[0]


def reference(x, dy, wq, wk, wv, wo, w_gate, w_up, w_down, m_wq, m_wk, m_wv, m_wo, m_w_gate, m_w_up, m_w_down, v_wq, v_wk, v_wv, v_wo, v_w_gate, v_w_up, v_w_down):
    weights = dict(zip(NAMES, (wq, wk, wv, wo, w_gate, w_up, w_down), strict=True))

    def take(so_far, sequence):
        h, by_y = sequence
        _, back = jax.vjp(stack, weights, h)
        by_weights, by_h = back(by_y)
        return jax.tree.map(lambda total, term: total + term.astype(jnp.float32), so_far, by_weights), by_h

    none_yet = {name: jnp.zeros(w.shape, jnp.float32) for name, w in weights.items()}
    by_weights, by_x = lax.scan(take, none_yet, (x, dy))
    gradients = [by_weights[name].astype(jnp.bfloat16).astype(jnp.float32) for name in NAMES]
    first = (m_wq, m_wk, m_wv, m_wo, m_w_gate, m_w_up, m_w_down)
    second = (v_wq, v_wk, v_wv, v_wo, v_w_gate, v_w_up, v_w_down)
    new = [adamw(weights[name].astype(jnp.float32), m, v, g) for name, m, v, g in zip(NAMES, first, second, gradients, strict=True)]
    return tuple(one[which] for which in range(3) for one in new)
```

```python
import functools

import jax
import jax.numpy as jnp
from jax import lax
from jax.experimental import pallas as pl
from jax.experimental.pallas import tpu as pltpu
from jax.sharding import PartitionSpec as P

HEAD = 256
THETA = 10000
EPS = 1e-6
HIDDEN = -2e30
LOG2E = 1.4426950408889634
LN2 = 0.6931471805599453
VMEM = 62 * 2**20
STRIP = 512
ROWS = 512
LOW = jnp.bfloat16
F32 = jnp.float32
ORDER = (3, 4, 5, 6, 0, 1, 2)


def dot(a, b, ca=1, cb=0):
    return lax.dot_general(a, b, (((ca,), (cb,)), ((), ())), preferred_element_type=F32)


def params(*semantics, **more):
    return pltpu.CompilerParams(dimension_semantics=semantics, vmem_limit_bytes=VMEM, **more)


def cost(flops, *arrays):
    return pl.CostEstimate(flops=int(flops), transcendentals=0, bytes_accessed=sum(a.size * a.dtype.itemsize for a in arrays))


def spread(h):
    wide = h.astype(F32)
    return wide, lax.rsqrt(jnp.mean(wide * wide, -1, keepdims=True) + EPS)


def norm_back(wide, scale, by):
    return scale * by - wide * (scale * scale * scale * jnp.mean(by * wide, -1, keepdims=True))


def turn(t, cos, sin):
    half, out = HEAD // 2, []
    for at in range(0, t.shape[1], HEAD):
        a, b = t[:, at : at + half].astype(F32), t[:, at + half : at + HEAD].astype(F32)
        out += [a * cos - b * sin, b * cos + a * sin]
    return jnp.concatenate(out, -1).astype(LOW)


def queries_keys_values(h, wq, wk, wv, cos, sin, q_ref, k_ref, v_ref):
    wide, scale = spread(h)
    a = (wide * scale).astype(LOW)
    q_ref[...] = turn(dot(a, wq[0]).astype(LOW), cos[...], sin[...])
    k_ref[...] = turn(dot(a, wk[0]).astype(LOW), cos[...], sin[...])
    v_ref[...] = dot(a, wv[0]).astype(LOW)


def matrix(w, layer):
    return pl.BlockSpec((1,) + w.shape[1:], lambda *_: (layer, 0, 0), pipeline_mode=pl.Buffered(1))


def rows(width, at=ROWS):
    return pl.BlockSpec((at, width), lambda i: (i, 0))


def first_kernel(h, wq, wk, wv, cos, sin, q_ref, k_ref, v_ref):
    queries_keys_values(h[...], wq, wk, wv, cos, sin, q_ref, k_ref, v_ref)


def first(h, wq, wk, wv, cos, sin, layer):
    t, d = h.shape
    n = wq.shape[2]
    outs = [jax.ShapeDtypeStruct((t, n), LOW)] * 3
    return pl.pallas_call(
        first_kernel,
        grid=(t // ROWS,),
        in_specs=[rows(d), matrix(wq, layer), matrix(wk, layer), matrix(wv, layer), rows(HEAD // 2), rows(HEAD // 2)],
        out_specs=[rows(n)] * 3,
        out_shape=outs,
        compiler_params=params("arbitrary"),
        cost_estimate=cost(6 * t * d * n, h, *outs),
        name="qkv",
    )(h, wq, wk, wv, cos, sin)


def mlp_chunk(b, wg, wu, at, size):
    gate = dot(b, wg[0, :, at : at + size])
    up = dot(b, wu[0, :, at : at + size])
    return gate, up, 0.5 * jnp.tanh(0.5 * gate) + 0.5


def middle_kernel(ctx, h, wo, wg, wu, wd, wq, wk, wv, cos, sin, out_ref, q_ref, k_ref, v_ref):
    h1 = (h[...].astype(F32) + dot(ctx[...], wo[0]).astype(LOW).astype(F32)).astype(LOW)
    wide, scale = spread(h1)
    b = (wide * scale).astype(LOW)
    ff, size = wg.shape[2], 512
    acts = []
    for at in range(0, ff, size):
        gate, up, s = mlp_chunk(b, wg, wu, at, size)
        acts.append((gate * s * up).astype(LOW))
    down = dot(jnp.concatenate(acts, -1), wd[0])
    h2 = (wide + down.astype(LOW).astype(F32)).astype(LOW)
    out_ref[...] = h2
    queries_keys_values(h2, wq, wk, wv, cos, sin, q_ref, k_ref, v_ref)


def middle(ctx, h, wo, wg, wu, wd, wq, wk, wv, cos, sin, layer):
    t, d = h.shape
    n, ff = wq.shape[2], wg.shape[2]
    outs = [jax.ShapeDtypeStruct((t, d), LOW)] + [jax.ShapeDtypeStruct((t, n), LOW)] * 3
    return pl.pallas_call(
        middle_kernel,
        grid=(t // ROWS,),
        in_specs=[rows(n), rows(d)] + [matrix(w, layer) for w in (wo, wg, wu, wd)] + [matrix(w, layer + 1) for w in (wq, wk, wv)]
        + [rows(HEAD // 2)] * 2,
        out_specs=[rows(d)] + [rows(n)] * 3,
        out_shape=outs,
        compiler_params=params("arbitrary"),
        cost_estimate=cost(2 * t * d * (4 * n + 3 * ff), h, h, *outs),
        name="middle",
    )(ctx, h, wo, wg, wu, wd, wq, wk, wv, cos, sin)


def causal_mask(size):
    return lax.broadcasted_iota(jnp.int32, (size, size), 1) >= lax.broadcasted_iota(jnp.int32, (size, size), 0)


def attention_kernel(q_ref, k_ref, v_ref, o_ref, lse_ref, mix_s, top_s):
    t, d = q_ref.shape
    e = d**-0.5 * LOG2E
    ones = jnp.ones((8, STRIP), LOW)
    blocks = [pl.ds(at, STRIP) for at in range(0, t, STRIP)]
    for j, keys in enumerate(blocks):
        k = k_ref[keys, :]
        values = jnp.concatenate([v_ref[keys, :].T, ones], axis=0)
        seen = blocks[j:]
        scores = [dot(k, q_ref[qs, :], 1, 1) for qs in seen]
        weights, keeps = [], []
        for qs, s in zip(seen, scores):
            if qs is keys:
                s = jnp.where(causal_mask(STRIP), s, HIDDEN)
            top = s.max(axis=0, keepdims=True)
            if j:
                old = top_s[0:1, qs]
                top = jnp.maximum(old, top)
                keeps.append(jnp.exp2((old - top) * e))
            top_s[0:1, qs] = top
            weights.append(jnp.exp2((s - top) * e).astype(LOW))
        for n, (qs, p) in enumerate(zip(seen, weights)):
            new = dot(values, p, 1, 0)
            if j:
                new = mix_s[:, qs] * keeps[n] + new
            if qs is keys:
                total = new[d : d + 1, :]
                o_ref[qs, :] = (new[:d, :] * (1 / total)).T.astype(LOW)
                lse_ref[0, :, qs] = top_s[0:1, qs] * e + jnp.log(total) * LOG2E
            else:
                mix_s[:, qs] = new


def head_specs(t, count):
    return [pl.BlockSpec((t, HEAD), lambda i: (0, i))] * count


def attention(q, k, v):
    t, n = q.shape
    outs = [jax.ShapeDtypeStruct((t, n), LOW), jax.ShapeDtypeStruct((n // HEAD, 1, t), F32)]
    return pl.pallas_call(
        attention_kernel,
        grid=(n // HEAD,),
        in_specs=head_specs(t, 3),
        out_specs=[*head_specs(t, 1), pl.BlockSpec((1, 1, t), lambda i: (i, 0, 0))],
        out_shape=outs,
        scratch_shapes=[pltpu.VMEM((HEAD + 8, t), F32), pltpu.VMEM((8, t), F32)],
        compiler_params=params("arbitrary"),
        cost_estimate=cost(2.5 * t * t * n, q, k, v, *outs),
        name="attention",
    )(q, k, v)


def attention_back_kernel(q_ref, k_ref, v_ref, do_ref, o_ref, lse_ref, dq_ref, dk_ref, dv_ref, dq_s):
    t, d = q_ref.shape
    scale = d**-0.5
    e = scale * LOG2E
    blocks = [pl.ds(at, STRIP) for at in range(0, t, STRIP)]
    deltas = []
    for qs in blocks:
        both = do_ref[qs, :].astype(F32) * o_ref[qs, :].astype(F32)
        folded = sum(both[:, at : at + 128] for at in range(0, d, 128))
        deltas.append(folded.T.sum(axis=0, keepdims=True))
    for j, keys in enumerate(blocks):
        k, v = k_ref[keys, :], v_ref[keys, :]
        kt = k.T
        seen = list(enumerate(blocks))[j:]
        scores = [dot(k, q_ref[qs, :], 1, 1) for _, qs in seen]
        dps = [dot(v, do_ref[qs, :], 1, 1) for _, qs in seen]
        ps, dss = [], []
        for m, (n, qs) in enumerate(seen):
            p = jnp.exp2(scores[m] * e - lse_ref[0, :, qs])
            if n == j:
                p = jnp.where(causal_mask(STRIP), p, 0.0)
            ds = (p * (dps[m] - deltas[n])).astype(LOW)
            ps.append(p.astype(LOW))
            dss.append(ds)
            new = dot(kt, ds, 1, 0)
            if j:
                new = dq_s[:, qs] + new
            if n == j:
                dq_ref[qs, :] = (new * scale).T.astype(LOW)
            else:
                dq_s[:, qs] = new
        late = pl.ds(j * STRIP, t - j * STRIP)
        dv_ref[keys, :] = dot(jnp.concatenate(ps, axis=1), do_ref[late, :], 1, 0).astype(LOW)
        dk_ref[keys, :] = (dot(jnp.concatenate(dss, axis=1), q_ref[late, :], 1, 0) * scale).astype(LOW)


def attention_back(q, k, v, by, out, lse):
    t, n = q.shape
    outs = [jax.ShapeDtypeStruct((t, n), LOW)] * 3
    return pl.pallas_call(
        attention_back_kernel,
        grid=(n // HEAD,),
        in_specs=[*head_specs(t, 5), pl.BlockSpec((1, 1, t), lambda i: (i, 0, 0))],
        out_specs=head_specs(t, 3),
        out_shape=outs,
        scratch_shapes=[pltpu.VMEM((HEAD, t), F32)],
        compiler_params=params("arbitrary"),
        cost_estimate=cost(6.25 * t * t * n, q, k, v, by, out, *outs),
        name="attention_back",
    )(q, k, v, by, out, lse)


def mlp_back_kernel(ctx, h, by, wo, wg, wu, wd, by_h1, by_ctx, grads, acc_o, acc_g, acc_u, acc_d):
    step = pl.program_id(0)

    @pl.when(step == 0)
    def _():
        for acc in (acc_o, acc_g, acc_u, acc_d):
            acc[...] = jnp.zeros_like(acc)

    h1 = (h[...].astype(F32) + dot(ctx[...], wo[0]).astype(LOW).astype(F32)).astype(LOW)
    wide, scale = spread(h1)
    b = (wide * scale).astype(LOW)
    bt, dyt = b.T, by[...].T
    ff, size = wg.shape[2], 512
    by_b = jnp.zeros(wide.shape, F32)
    for at in range(0, ff, size):
        here = pl.ds(at, size)
        gate, up, s = mlp_chunk(b, wg, wu, at, size)
        by_act = dot(by[...], wd[0, here, :], 1, 1).astype(LOW).astype(F32)
        silu = gate * s
        act = (silu * up).astype(LOW)
        by_up = (by_act * silu).astype(LOW)
        by_gate = (by_act * up * (s + silu * (1.0 - s))).astype(LOW)
        by_b = by_b + dot(by_gate, wg[0, :, here], 1, 1) + dot(by_up, wu[0, :, here], 1, 1)
        acc_d[:, here] += dot(dyt, act)
        acc_g[:, here] += dot(bt, by_gate)
        acc_u[:, here] += dot(bt, by_up)
    total = (by[...].astype(F32) + norm_back(wide, scale, by_b.astype(LOW).astype(F32)).astype(LOW).astype(F32)).astype(LOW)
    by_h1[...] = total
    by_ctx[...] = dot(total, wo[0], 1, 1).astype(LOW)
    acc_o[...] += dot(ctx[...].T, total)

    @pl.when(step == pl.num_programs(0) - 1)
    def _():
        n, at = grads.shape[0], 0
        for acc in (acc_o, acc_g, acc_u):
            r = acc.shape[0] // n
            for c in range(0, acc.shape[1], 512):
                grads[:, at : at + r, :] = acc[:, c : c + 512].reshape(n, r, 512).astype(LOW)
                at += r
        r = ff // n
        for first_owner in range(0, n, max(512 // r, 1)):
            many = max(512 // r, 1) if n >= max(512 // r, 1) else n
            piece = acc_d[:, first_owner * r : (first_owner + many) * r].T
            grads[first_owner : first_owner + many, at : at + r, :] = piece.reshape(many, r, 512).astype(LOW)


def mlp_back(ctx, h, by, wo, wg, wu, wd, layer, n, size=256):
    t, d = h.shape
    heads, ff = wo.shape[1], wg.shape[2]
    packed = (heads * d + 3 * d * ff) // (512 * n)
    outs = [jax.ShapeDtypeStruct((t, d), LOW), jax.ShapeDtypeStruct((t, heads), LOW), jax.ShapeDtypeStruct((n, packed + 3 * d // n, 512), LOW)]
    return pl.pallas_call(
        mlp_back_kernel,
        grid=(t // size,),
        in_specs=[rows(heads, size), rows(d, size), rows(d, size)] + [matrix(w, layer) for w in (wo, wg, wu, wd)],
        out_specs=[rows(d, size), rows(heads, size), pl.BlockSpec((n, packed, 512), lambda i: (0, 0, 0), pipeline_mode=pl.Buffered(1))],
        out_shape=outs,
        scratch_shapes=[pltpu.VMEM((heads, d), F32)] + [pltpu.VMEM((d, ff), F32)] * 3,
        compiler_params=params("arbitrary"),
        cost_estimate=cost(2 * t * d * (8 * ff + 3 * heads), h, h, h, *outs),
        name="mlp_back",
    )(ctx, h, by, wo, wg, wu, wd)


def qkv_back_kernel(packed, dq, dk, dv, h, cos, sin, *rest, deeper):
    if deeper:
        by_h1, wq, wk, wv, by_h = rest[:5]
        rest = rest[5:]
    grads, acc_q, acc_k, acc_v, mine, sem = rest
    step = pl.program_id(0)

    @pl.when(step == 0)
    def _():
        for acc in (acc_q, acc_k, acc_v):
            acc[...] = jnp.zeros_like(acc)

    wide, scale = spread(h[...])
    at = (wide * scale).astype(LOW).T
    by_q, by_k = turn(dq[...], cos[...], -sin[...]), turn(dk[...], cos[...], -sin[...])
    acc_q[...] += dot(at, by_q)
    acc_k[...] += dot(at, by_k)
    acc_v[...] += dot(at, dv[...])
    if deeper:
        by_a = dot(by_q, wq[0], 1, 1) + dot(by_k, wk[0], 1, 1) + dot(dv[...], wv[0], 1, 1)
        by_h[...] = (by_h1[...].astype(F32) + norm_back(wide, scale, by_a.astype(LOW).astype(F32)).astype(LOW).astype(F32)).astype(LOW)

    @pl.when(step == pl.num_programs(0) - 1)
    def _():
        n = grads.shape[0]
        r = acc_q.shape[0] // n
        for i, acc in enumerate((acc_q, acc_k, acc_v)):
            mine[:, i * r : (i + 1) * r, :] = acc[...].reshape(n, r, 512).astype(LOW)
        copy = pltpu.make_async_copy(mine, grads.at[:, pl.ds(grads.shape[1] - 3 * r, 3 * r), :], sem)
        copy.start()
        copy.wait()


def qkv_back(packed, dq, dk, dv, h, cos, sin, layer, by_h1=None, wq=None, wk=None, wv=None):
    t, d = h.shape
    heads = dq.shape[1]
    deeper = by_h1 is not None
    n = packed.shape[0]
    outs = [jax.ShapeDtypeStruct(packed.shape, LOW)]
    out_specs = [pl.BlockSpec(memory_space=pl.ANY)]
    given, specs = [packed, dq, dk, dv, h, cos, sin], [pl.BlockSpec(memory_space=pl.ANY)] + [rows(heads)] * 3 + [rows(d)] + [rows(HEAD // 2)] * 2
    if deeper:
        given += [by_h1, wq, wk, wv]
        specs += [rows(d)] + [matrix(w, layer) for w in (wq, wk, wv)]
        outs = [jax.ShapeDtypeStruct((t, d), LOW)] + outs
        out_specs = [rows(d)] + out_specs
    return pl.pallas_call(
        functools.partial(qkv_back_kernel, deeper=deeper),
        grid=(t // ROWS,),
        in_specs=specs,
        out_specs=out_specs,
        out_shape=outs,
        scratch_shapes=[pltpu.VMEM((d, heads), F32)] * 3 + [pltpu.VMEM((n, 3 * d // n, heads), LOW), pltpu.SemaphoreType.DMA],
        input_output_aliases={0: len(outs) - 1},
        compiler_params=params("arbitrary"),
        cost_estimate=cost(2 * t * d * heads * (6 if deeper else 3), dq, dk, dv, h, *outs),
        name="qkv_back",
    )(*given)


def adamw_kernel(me, packed_g, *refs):
    ws, ms, vs = refs[:7], refs[7:14], refs[14:21]
    rest = refs[-15:]
    packed, new_m, new_v = rest[0], rest[1:8], rest[8:15]
    at = 0
    for i in ORDER:
        r, width = ms[i].shape[1], ms[i].shape[2]
        for c in range(0, width, 512):
            cols = slice(c, c + 512)
            g = packed_g[at : at + r, :].astype(F32)
            m = 0.9 * ms[i][0, :, cols] + 0.1 * g
            v = 0.95 * vs[i][0, :, cols] + 0.05 * g * g
            w = ws[i][0, :, cols].astype(F32)
            new_m[i][0, :, cols] = m
            new_v[i][0, :, cols] = v
            packed[at : at + r, :] = (w - 0.02 * (m * lax.rsqrt(v + 1e-8) + 0.1 * w)).astype(LOW)
            at += r


def adamw(me, g, ws, ms, vs, layer, earlier=()):
    own = [pl.BlockSpec((1,) + m.shape[1:], lambda i, me: (layer, me[0], 0)) for m in ms]
    part = [pl.BlockSpec((1,) + m.shape[1:], lambda i, me: (layer, 0, 0)) for m in ms]
    whole = lambda a: pl.BlockSpec(a.shape, lambda i, me: (0,) * a.ndim)
    total = g.shape[0]
    outs = [jax.ShapeDtypeStruct((total, 512), LOW)] + [jax.ShapeDtypeStruct(m.shape, F32) for m in (*ms, *vs)]
    given = [g, *ws, *ms, *vs, *earlier]
    return pl.pallas_call(
        adamw_kernel,
        grid_spec=pltpu.PrefetchScalarGridSpec(
            num_scalar_prefetch=1,
            grid=(1,),
            in_specs=[whole(g), *own, *part, *part] + [pl.BlockSpec(memory_space=pl.ANY)] * len(earlier),
            out_specs=[pl.BlockSpec((total, 512), lambda i, me: (0, 0)), *part, *part],
        ),
        out_shape=outs,
        input_output_aliases={1 + 1 + 21 + i: 1 + i for i in range(len(earlier))},
        compiler_params=params("arbitrary"),
        cost_estimate=cost(20 * total * 512, g, *outs),
        name="adamw",
    )(me, *given)


def unpack_kernel(*refs):
    packed, outs = refs[:-7], refs[-7:]
    for layer, p in enumerate(packed):
        at = 0
        for out in (outs[i] for i in ORDER):
            r = out.shape[1]
            for c in range(0, out.shape[2], 512):
                out[layer, :, c : c + 512] = p[0, at : at + r, :]
                at += r


def unpack(packed, ws, n):
    outs = [jax.ShapeDtypeStruct(w.shape, LOW) for w in ws]
    total = packed[0].shape[0] // n
    return pl.pallas_call(
        unpack_kernel,
        grid=(n,),
        in_specs=[pl.BlockSpec((1, total, 512), lambda i: (i, 0, 0))] * len(packed),
        out_specs=[pl.BlockSpec((w.shape[0], w.shape[1] // n, w.shape[2]), lambda i: (0, i, 0)) for w in ws],
        out_shape=outs,
        compiler_params=params("arbitrary"),
        cost_estimate=cost(0, *outs, *outs),
        name="unpack",
    )(*(p.reshape(n, total, 512) for p in packed))


def solution(mesh):
    n = mesh.shape["dp"]

    def scatter(g):
        return lax.psum_scatter(g.reshape(-1, g.shape[2]), "dp", scatter_dimension=0, tiled=True)

    def step(x, dy, *arrays):
        weights, m, v = (arrays[i : i + 7] for i in (0, 7, 14))
        wq, wk, wv, wo, wg, wu, wd = weights
        h0, t = x[0], x.shape[1]
        half = HEAD // 2
        angle = jnp.arange(t, dtype=F32)[:, None] * THETA ** (-jnp.arange(half, dtype=F32) / half)
        cos, sin = jnp.cos(angle), jnp.sin(angle)
        me = lax.axis_index("dp").astype(jnp.int32).reshape(1)
        q0, k0, v0 = first(h0, wq, wk, wv, cos, sin, 0)
        c0, l0 = attention(q0, k0, v0)
        h1, q1, k1, v1 = middle(c0, h0, wo, wg, wu, wd, wq, wk, wv, cos, sin, 0)
        c1, l1 = attention(q1, k1, v1)
        by, by_c, g1 = mlp_back(c1, h1, dy[0], wo, wg, wu, wd, 1, n)
        dq, dk, dv = attention_back(q1, k1, v1, by_c, c1, l1)
        by, g1 = qkv_back(g1, dq, dk, dv, h1, cos, sin, 1, by, wq, wk, wv)
        r1 = scatter(g1)
        by, by_c, g0 = mlp_back(c0, h0, by, wo, wg, wu, wd, 0, n)
        dq, dk, dv = attention_back(q0, k0, v0, by_c, c0, l0)
        (g0,) = qkv_back(g0, dq, dk, dv, h0, cos, sin, 0)
        r0 = scatter(g0)
        new1, *moments = adamw(me, r1, weights, m, v, 1)
        all1 = lax.all_gather(new1, "dp", axis=0, tiled=True)
        new0, *moments = adamw(me, r0, weights, m, v, 0, moments)
        all0 = lax.all_gather(new0, "dp", axis=0, tiled=True)
        return (*unpack((all0, all1), weights, n), *moments)

    states, all_of, cut = P(("rep", "dp"), None, None), P(None, None, None), P(None, "dp", None)
    return jax.shard_map(
        step,
        mesh=mesh,
        in_specs=(states, states) + (all_of,) * 7 + (cut,) * 14,
        out_specs=(P("rep", None, None),) * 7 + (P("rep", "dp", None),) * 14,
        check_vma=False,
    )
```

```python
import functools

import jax
import jax.numpy as jnp
from jax import lax
from jax.experimental import pallas as pl
from jax.experimental.pallas import tpu as pltpu
from jax.sharding import PartitionSpec as P

HEAD = 256
THETA = 10000
EPS = 1e-6
HIDDEN = -2e30
LOG2E = 1.4426950408889634
LN2 = 0.6931471805599453
VMEM = 62 * 2**20
STRIP = 512
ROWS = 512
LOW = jnp.bfloat16
F32 = jnp.float32
ORDER = (3, 4, 5, 6, 0, 1, 2)


def dot(a, b, ca=1, cb=0):
    return lax.dot_general(a, b, (((ca,), (cb,)), ((), ())), preferred_element_type=F32)


def params(*semantics, **more):
    return pltpu.CompilerParams(dimension_semantics=semantics, vmem_limit_bytes=VMEM, **more)


def cost(flops, *arrays):
    return pl.CostEstimate(flops=int(flops), transcendentals=0, bytes_accessed=sum(a.size * a.dtype.itemsize for a in arrays))


def spread(h):
    wide = h.astype(F32)
    return wide, lax.rsqrt(jnp.mean(wide * wide, -1, keepdims=True) + EPS)


def norm_back(wide, scale, by):
    return scale * by - wide * (scale * scale * scale * jnp.mean(by * wide, -1, keepdims=True))


def turn(t, cos, sin):
    half, out = HEAD // 2, []
    for at in range(0, t.shape[1], HEAD):
        a, b = t[:, at : at + half].astype(F32), t[:, at + half : at + HEAD].astype(F32)
        out += [a * cos - b * sin, b * cos + a * sin]
    return jnp.concatenate(out, -1).astype(LOW)


def queries_keys_values(h, wq, wk, wv, cos, sin, q_ref, k_ref, v_ref):
    wide, scale = spread(h)
    a = (wide * scale).astype(LOW)
    q_ref[...] = turn(dot(a, wq[0]).astype(LOW), cos[...], sin[...])
    k_ref[...] = turn(dot(a, wk[0]).astype(LOW), cos[...], sin[...])
    v_ref[...] = dot(a, wv[0]).astype(LOW)


def matrix(w, layer):
    return pl.BlockSpec((1,) + w.shape[1:], lambda *_: (layer, 0, 0), pipeline_mode=pl.Buffered(1))


def rows(width, at=ROWS):
    return pl.BlockSpec((at, width), lambda i: (i, 0))


def first_kernel(h, wq, wk, wv, cos, sin, q_ref, k_ref, v_ref):
    queries_keys_values(h[...], wq, wk, wv, cos, sin, q_ref, k_ref, v_ref)


def first(h, wq, wk, wv, cos, sin, layer):
    t, d = h.shape
    n = wq.shape[2]
    outs = [jax.ShapeDtypeStruct((t, n), LOW)] * 3
    return pl.pallas_call(
        first_kernel,
        grid=(t // ROWS,),
        in_specs=[rows(d), matrix(wq, layer), matrix(wk, layer), matrix(wv, layer), rows(HEAD // 2), rows(HEAD // 2)],
        out_specs=[rows(n)] * 3,
        out_shape=outs,
        compiler_params=params("arbitrary"),
        cost_estimate=cost(6 * t * d * n, h, *outs),
        name="qkv",
    )(h, wq, wk, wv, cos, sin)


def mlp_chunk(b, wg, wu, at, size):
    gate = dot(b, wg[0, :, at : at + size])
    up = dot(b, wu[0, :, at : at + size])
    return gate, up, 0.5 * jnp.tanh(0.5 * gate) + 0.5


def middle_kernel(ctx, h, wo, wg, wu, wd, wq, wk, wv, cos, sin, out_ref, q_ref, k_ref, v_ref):
    h1 = (h[...].astype(F32) + dot(ctx[...], wo[0]).astype(LOW).astype(F32)).astype(LOW)
    wide, scale = spread(h1)
    b = (wide * scale).astype(LOW)
    ff, size = wg.shape[2], 512
    acts = []
    for at in range(0, ff, size):
        gate, up, s = mlp_chunk(b, wg, wu, at, size)
        acts.append((gate * s * up).astype(LOW))
    down = dot(jnp.concatenate(acts, -1), wd[0])
    h2 = (wide + down.astype(LOW).astype(F32)).astype(LOW)
    out_ref[...] = h2
    queries_keys_values(h2, wq, wk, wv, cos, sin, q_ref, k_ref, v_ref)


def middle(ctx, h, wo, wg, wu, wd, wq, wk, wv, cos, sin, layer):
    t, d = h.shape
    n, ff = wq.shape[2], wg.shape[2]
    outs = [jax.ShapeDtypeStruct((t, d), LOW)] + [jax.ShapeDtypeStruct((t, n), LOW)] * 3
    return pl.pallas_call(
        middle_kernel,
        grid=(t // ROWS,),
        in_specs=[rows(n), rows(d)] + [matrix(w, layer) for w in (wo, wg, wu, wd)] + [matrix(w, layer + 1) for w in (wq, wk, wv)]
        + [rows(HEAD // 2)] * 2,
        out_specs=[rows(d)] + [rows(n)] * 3,
        out_shape=outs,
        compiler_params=params("arbitrary"),
        cost_estimate=cost(2 * t * d * (4 * n + 3 * ff), h, h, *outs),
        name="middle",
    )(ctx, h, wo, wg, wu, wd, wq, wk, wv, cos, sin)


def causal_mask(size):
    return lax.broadcasted_iota(jnp.int32, (size, size), 1) >= lax.broadcasted_iota(jnp.int32, (size, size), 0)


def attention_kernel(q_ref, k_ref, v_ref, o_ref, lse_ref, mix_s, top_s):
    t, d = q_ref.shape
    e = d**-0.5 * LOG2E
    ones = jnp.ones((8, STRIP), LOW)
    blocks = [pl.ds(at, STRIP) for at in range(0, t, STRIP)]
    for j, keys in enumerate(blocks):
        k = k_ref[keys, :]
        values = jnp.concatenate([v_ref[keys, :].T, ones], axis=0)
        seen = blocks[j:]
        scores = [dot(k, q_ref[qs, :], 1, 1) for qs in seen]
        weights, keeps = [], []
        for qs, s in zip(seen, scores):
            if qs is keys:
                s = jnp.where(causal_mask(STRIP), s, HIDDEN)
            top = s.max(axis=0, keepdims=True)
            if j:
                old = top_s[0:1, qs]
                top = jnp.maximum(old, top)
                keeps.append(jnp.exp2((old - top) * e))
            top_s[0:1, qs] = top
            weights.append(jnp.exp2((s - top) * e).astype(LOW))
        for n, (qs, p) in enumerate(zip(seen, weights)):
            new = dot(values, p, 1, 0)
            if j:
                new = mix_s[:, qs] * keeps[n] + new
            if qs is keys:
                total = new[d : d + 1, :]
                o_ref[qs, :] = (new[:d, :] * (1 / total)).T.astype(LOW)
                lse_ref[0, :, qs] = top_s[0:1, qs] * e + jnp.log(total) * LOG2E
            else:
                mix_s[:, qs] = new


def head_specs(t, count):
    return [pl.BlockSpec((t, HEAD), lambda i: (0, i))] * count


def attention(q, k, v):
    t, n = q.shape
    outs = [jax.ShapeDtypeStruct((t, n), LOW), jax.ShapeDtypeStruct((n // HEAD, 1, t), F32)]
    return pl.pallas_call(
        attention_kernel,
        grid=(n // HEAD,),
        in_specs=head_specs(t, 3),
        out_specs=[*head_specs(t, 1), pl.BlockSpec((1, 1, t), lambda i: (i, 0, 0))],
        out_shape=outs,
        scratch_shapes=[pltpu.VMEM((HEAD + 8, t), F32), pltpu.VMEM((8, t), F32)],
        compiler_params=params("arbitrary"),
        cost_estimate=cost(2.5 * t * t * n, q, k, v, *outs),
        name="attention",
    )(q, k, v)


def attention_back_kernel(q_ref, k_ref, v_ref, do_ref, o_ref, lse_ref, dq_ref, dk_ref, dv_ref, dq_s):
    t, d = q_ref.shape
    scale = d**-0.5
    e = scale * LOG2E
    blocks = [pl.ds(at, STRIP) for at in range(0, t, STRIP)]
    deltas = []
    for qs in blocks:
        both = do_ref[qs, :].astype(F32) * o_ref[qs, :].astype(F32)
        folded = sum(both[:, at : at + 128] for at in range(0, d, 128))
        deltas.append(folded.T.sum(axis=0, keepdims=True))
    for j, keys in enumerate(blocks):
        k, v = k_ref[keys, :], v_ref[keys, :]
        kt = k.T
        seen = list(enumerate(blocks))[j:]
        scores = [dot(k, q_ref[qs, :], 1, 1) for _, qs in seen]
        dps = [dot(v, do_ref[qs, :], 1, 1) for _, qs in seen]
        ps, dss = [], []
        for m, (n, qs) in enumerate(seen):
            p = jnp.exp2(scores[m] * e - lse_ref[0, :, qs])
            if n == j:
                p = jnp.where(causal_mask(STRIP), p, 0.0)
            ds = (p * (dps[m] - deltas[n])).astype(LOW)
            ps.append(p.astype(LOW))
            dss.append(ds)
            new = dot(kt, ds, 1, 0)
            if j:
                new = dq_s[:, qs] + new
            if n == j:
                dq_ref[qs, :] = (new * scale).T.astype(LOW)
            else:
                dq_s[:, qs] = new
        late = pl.ds(j * STRIP, t - j * STRIP)
        dv_ref[keys, :] = dot(jnp.concatenate(ps, axis=1), do_ref[late, :], 1, 0).astype(LOW)
        dk_ref[keys, :] = (dot(jnp.concatenate(dss, axis=1), q_ref[late, :], 1, 0) * scale).astype(LOW)


def attention_back(q, k, v, by, out, lse):
    t, n = q.shape
    outs = [jax.ShapeDtypeStruct((t, n), LOW)] * 3
    return pl.pallas_call(
        attention_back_kernel,
        grid=(n // HEAD,),
        in_specs=[*head_specs(t, 5), pl.BlockSpec((1, 1, t), lambda i: (i, 0, 0))],
        out_specs=head_specs(t, 3),
        out_shape=outs,
        scratch_shapes=[pltpu.VMEM((HEAD, t), F32)],
        compiler_params=params("arbitrary"),
        cost_estimate=cost(6.25 * t * t * n, q, k, v, by, out, *outs),
        name="attention_back",
    )(q, k, v, by, out, lse)


def mlp_back_kernel(ctx, h, by, wo, wg, wu, wd, by_h1, by_ctx, grads, acc_o, acc_g, acc_u, acc_d):
    step = pl.program_id(0)

    @pl.when(step == 0)
    def _():
        for acc in (acc_o, acc_g, acc_u, acc_d):
            acc[...] = jnp.zeros_like(acc)

    h1 = (h[...].astype(F32) + dot(ctx[...], wo[0]).astype(LOW).astype(F32)).astype(LOW)
    wide, scale = spread(h1)
    b = (wide * scale).astype(LOW)
    bt, dyt = b.T, by[...].T
    ff, size = wg.shape[2], 512
    by_b = jnp.zeros(wide.shape, F32)
    for at in range(0, ff, size):
        here = pl.ds(at, size)
        gate, up, s = mlp_chunk(b, wg, wu, at, size)
        by_act = dot(by[...], wd[0, here, :], 1, 1).astype(LOW).astype(F32)
        silu = gate * s
        act = (silu * up).astype(LOW)
        by_up = (by_act * silu).astype(LOW)
        by_gate = (by_act * up * (s + silu * (1.0 - s))).astype(LOW)
        by_b = by_b + dot(by_gate, wg[0, :, here], 1, 1) + dot(by_up, wu[0, :, here], 1, 1)
        acc_d[:, here] += dot(dyt, act)
        acc_g[:, here] += dot(bt, by_gate)
        acc_u[:, here] += dot(bt, by_up)
    total = (by[...].astype(F32) + norm_back(wide, scale, by_b.astype(LOW).astype(F32)).astype(LOW).astype(F32)).astype(LOW)
    by_h1[...] = total
    by_ctx[...] = dot(total, wo[0], 1, 1).astype(LOW)
    acc_o[...] += dot(ctx[...].T, total)

    @pl.when(step == pl.num_programs(0) - 1)
    def _():
        n, at = grads.shape[0], 0
        for acc in (acc_o, acc_g, acc_u):
            r = acc.shape[0] // n
            for c in range(0, acc.shape[1], 512):
                grads[:, at : at + r, :] = acc[:, c : c + 512].reshape(n, r, 512).astype(LOW)
                at += r
        r = ff // n
        for first_owner in range(0, n, max(512 // r, 1)):
            many = max(512 // r, 1) if n >= max(512 // r, 1) else n
            piece = acc_d[:, first_owner * r : (first_owner + many) * r].T
            grads[first_owner : first_owner + many, at : at + r, :] = piece.reshape(many, r, 512).astype(LOW)


def mlp_back(ctx, h, by, wo, wg, wu, wd, layer, n, size=512):
    t, d = h.shape
    heads, ff = wo.shape[1], wg.shape[2]
    packed = (heads * d + 3 * d * ff) // (512 * n)
    outs = [jax.ShapeDtypeStruct((t, d), LOW), jax.ShapeDtypeStruct((t, heads), LOW), jax.ShapeDtypeStruct((n, packed + 3 * d // n, 512), LOW)]
    return pl.pallas_call(
        mlp_back_kernel,
        grid=(t // size,),
        in_specs=[rows(heads, size), rows(d, size), rows(d, size)] + [matrix(w, layer) for w in (wo, wg, wu, wd)],
        out_specs=[rows(d, size), rows(heads, size), pl.BlockSpec((n, packed, 512), lambda i: (0, 0, 0), pipeline_mode=pl.Buffered(1))],
        out_shape=outs,
        scratch_shapes=[pltpu.VMEM((heads, d), F32)] + [pltpu.VMEM((d, ff), F32)] * 3,
        compiler_params=params("arbitrary"),
        cost_estimate=cost(2 * t * d * (8 * ff + 3 * heads), h, h, h, *outs),
        name="mlp_back",
    )(ctx, h, by, wo, wg, wu, wd)


def qkv_back_kernel(packed, dq, dk, dv, h, cos, sin, *rest, deeper, after):
    if deeper:
        by_h1, wq, wk, wv = rest[:4]
        rest = rest[4:]
    rest = rest[after:]
    if deeper:
        by_h, rest = rest[0], rest[1:]
    grads, acc_q, acc_k, acc_v, mine, sem = rest
    step = pl.program_id(0)

    @pl.when(step == 0)
    def _():
        for acc in (acc_q, acc_k, acc_v):
            acc[...] = jnp.zeros_like(acc)

    wide, scale = spread(h[...])
    at = (wide * scale).astype(LOW).T
    by_q, by_k = turn(dq[...], cos[...], -sin[...]), turn(dk[...], cos[...], -sin[...])
    acc_q[...] += dot(at, by_q)
    acc_k[...] += dot(at, by_k)
    acc_v[...] += dot(at, dv[...])
    if deeper:
        by_a = dot(by_q, wq[0], 1, 1) + dot(by_k, wk[0], 1, 1) + dot(dv[...], wv[0], 1, 1)
        by_h[...] = (by_h1[...].astype(F32) + norm_back(wide, scale, by_a.astype(LOW).astype(F32)).astype(LOW).astype(F32)).astype(LOW)

    @pl.when(step == pl.num_programs(0) - 1)
    def _():
        n = grads.shape[0]
        r = acc_q.shape[0] // n
        for i, acc in enumerate((acc_q, acc_k, acc_v)):
            mine[:, i * r : (i + 1) * r, :] = acc[...].reshape(n, r, 512).astype(LOW)
        copy = pltpu.make_async_copy(mine, grads.at[:, pl.ds(grads.shape[1] - 3 * r, 3 * r), :], sem)
        copy.start()
        copy.wait()


def qkv_back(packed, dq, dk, dv, h, cos, sin, layer, by_h1=None, wq=None, wk=None, wv=None, after=()):
    t, d = h.shape
    heads = dq.shape[1]
    deeper = by_h1 is not None
    n = packed.shape[0]
    outs = [jax.ShapeDtypeStruct(packed.shape, LOW)]
    out_specs = [pl.BlockSpec(memory_space=pl.ANY)]
    given, specs = [packed, dq, dk, dv, h, cos, sin], [pl.BlockSpec(memory_space=pl.ANY)] + [rows(heads)] * 3 + [rows(d)] + [rows(HEAD // 2)] * 2
    if deeper:
        given += [by_h1, wq, wk, wv]
        specs += [rows(d)] + [matrix(w, layer) for w in (wq, wk, wv)]
        outs = [jax.ShapeDtypeStruct((t, d), LOW)] + outs
        out_specs = [rows(d)] + out_specs
    given += list(after)
    specs += [pl.BlockSpec(memory_space=pl.ANY)] * len(after)
    return pl.pallas_call(
        functools.partial(qkv_back_kernel, deeper=deeper, after=len(after)),
        grid=(t // ROWS,),
        in_specs=specs,
        out_specs=out_specs,
        out_shape=outs,
        scratch_shapes=[pltpu.VMEM((d, heads), F32)] * 3 + [pltpu.VMEM((n, 3 * d // n, heads), LOW), pltpu.SemaphoreType.DMA],
        input_output_aliases={0: len(outs) - 1},
        compiler_params=params("arbitrary"),
        cost_estimate=cost(2 * t * d * heads * (6 if deeper else 3), dq, dk, dv, h, *outs),
        name="qkv_back",
    )(*given)


def adamw_kernel(me, packed_g, *refs):
    ws, ms, vs = refs[:7], refs[7:14], refs[14:21]
    rest = refs[-15:]
    packed, new_m, new_v = rest[0], rest[1:8], rest[8:15]
    at = 0
    for i in ORDER:
        r, width = ms[i].shape[1], ms[i].shape[2]
        for c in range(0, width, 512):
            cols = slice(c, c + 512)
            g = packed_g[at : at + r, :].astype(F32)
            m = 0.9 * ms[i][0, :, cols] + 0.1 * g
            v = 0.95 * vs[i][0, :, cols] + 0.05 * g * g
            w = ws[i][0, :, cols].astype(F32)
            new_m[i][0, :, cols] = m
            new_v[i][0, :, cols] = v
            packed[at : at + r, :] = (w - 0.02 * (m * lax.rsqrt(v + 1e-8) + 0.1 * w)).astype(LOW)
            at += r


def adamw(me, g, ws, ms, vs, layer, earlier=(), after=()):
    own = [pl.BlockSpec((1,) + m.shape[1:], lambda i, me: (layer, me[0], 0)) for m in ms]
    part = [pl.BlockSpec((1,) + m.shape[1:], lambda i, me: (layer, 0, 0)) for m in ms]
    whole = lambda a: pl.BlockSpec(a.shape, lambda i, me: (0,) * a.ndim)
    total = g.shape[0]
    outs = [jax.ShapeDtypeStruct((total, 512), LOW)] + [jax.ShapeDtypeStruct(m.shape, F32) for m in (*ms, *vs)]
    given = [g, *ws, *ms, *vs, *earlier, *after]
    return pl.pallas_call(
        adamw_kernel,
        grid_spec=pltpu.PrefetchScalarGridSpec(
            num_scalar_prefetch=1,
            grid=(1,),
            in_specs=[whole(g), *own, *part, *part] + [pl.BlockSpec(memory_space=pl.ANY)] * len([*earlier, *after]),
            out_specs=[pl.BlockSpec((total, 512), lambda i, me: (0, 0)), *part, *part],
        ),
        out_shape=outs,
        input_output_aliases={1 + 1 + 21 + i: 1 + i for i in range(len(earlier))},
        compiler_params=params("arbitrary"),
        cost_estimate=cost(20 * total * 512, g, *outs),
        name="adamw",
    )(me, *given)


def unpack_kernel(packed, *refs):
    at = 0
    for out in (refs[-7:][i] for i in ORDER):
        owners = packed.shape[0]
        r = out.shape[1] // owners
        for c in range(0, out.shape[2], 512):
            for owner in range(owners):
                out[0, owner * r : (owner + 1) * r, c : c + 512] = packed[owner, at : at + r, :]
            at += r


def unpack(packed, ws, n, layer, earlier=()):
    outs = [jax.ShapeDtypeStruct(w.shape, LOW) for w in ws]
    total = packed.shape[0] // n
    some = min(n, 4)
    return pl.pallas_call(
        unpack_kernel,
        grid=(n // some,),
        in_specs=[pl.BlockSpec((some, total, 512), lambda i: (i, 0, 0))] + [pl.BlockSpec(memory_space=pl.ANY)] * len(earlier),
        out_specs=[pl.BlockSpec((1, some * w.shape[1] // n, w.shape[2]), lambda i: (layer, i, 0)) for w in ws],
        out_shape=outs,
        input_output_aliases={1 + i: i for i in range(len(earlier))},
        compiler_params=params("arbitrary"),
        cost_estimate=cost(0, *outs),
        name="unpack",
    )(packed.reshape(n, total, 512), *earlier)


CORES = 2
PARTS = 4


def reduce_kernel(g, out, mine, pair, sent, got, mine_sem, pair_send, pair_got, send_sem, got_sem):
    n, total = g.shape[0], g.shape[1]
    chips = n // CORES
    far, size = chips // 2, total // PARTS
    me = lax.axis_index("dp")
    z, core = lax.div(me, CORES), lax.rem(me, CORES)
    at = lambda chip, which: {"dp": lax.rem(chip + chips, chips) * CORES + which}
    peers = {1: at(z + 1, core), -1: at(z - 1, core)}
    partner = at(z, 1 - core)

    barrier = pltpu.get_barrier_semaphore()
    for peer in (peers[1], peers[-1], partner):
        pl.semaphore_signal(barrier, inc=1, device_id=peer, device_id_type=pl.DeviceIdType.MESH)

    order = [far] + [x * sign for x in range(far - 1, 0, -1) for sign in (1, -1)] + [0]
    slot = {offset: i for i, offset in enumerate(order)} | {-far: 0}
    local = []
    for i, offset in enumerate(order):
        chunk = lax.rem(z + offset + chips, chips) * CORES
        local.append(pltpu.make_async_copy(g.at[chunk + core], mine.at[i], mine_sem.at[i]))
        local[i].start()
    pl.semaphore_wait(barrier, 3)
    across = []
    for i, offset in enumerate(order):
        chunk = lax.rem(z + offset + chips, chips) * CORES
        across.append(pltpu.make_async_remote_copy(g.at[chunk + 1 - core], pair.at[i], pair_send.at[i], pair_got.at[i], device_id=partner,
                                                   device_id_type=pl.DeviceIdType.MESH))
        across[i].start()

    streams = [(sign, part, far if (part < PARTS // 2) == (sign > 0) else far - 1) for part in range(PARTS) for sign in (1, -1)]
    ready, copies = set(), {}

    def own(offset, here):
        i = slot[offset]
        if i not in ready:
            ready.add(i)
            local[i].wait()
            across[i].wait_recv()
        return mine[i, here, :].astype(F32) + pair[i, here, :].astype(F32)

    for s in range(far):
        pending = None
        for x, (sign, part, hops) in enumerate(streams):
            if s < hops:
                value = own(sign * (hops - s), pl.ds(part * size, size))
                if s:
                    copies[s - 1, x].wait_recv()
                    value = value + got[s - 1, x].astype(F32)
                sent[s, x] = value.astype(LOW)
                copies[s, x] = pltpu.make_async_remote_copy(sent.at[s, x], got.at[s, x], send_sem.at[s, x], got_sem.at[s, x],
                                                            device_id=peers[sign], device_id_type=pl.DeviceIdType.MESH)
                if pending is not None:
                    pending.start()
                pending = copies[s, x]
        pending.start()
    for part in range(PARTS):
        here = pl.ds(part * size, size)
        value = own(0, here)
        for x, (_, of, hops) in enumerate(streams):
            if of == part:
                copies[hops - 1, x].wait_recv()
                value = value + got[hops - 1, x].astype(F32)
        out[here, :] = value.astype(LOW)
    for copy in (*across, *copies.values()):
        copy.wait_send()


def reduce(g):
    n, total, width = g.shape
    chips = n // CORES
    far, streams = chips // 2, 2 * PARTS
    out = jax.ShapeDtypeStruct((total, width), LOW)
    dma = lambda *shape: pltpu.SemaphoreType.DMA(shape)
    return pl.pallas_call(
        reduce_kernel,
        in_specs=[pl.BlockSpec(memory_space=pl.ANY)],
        out_specs=pl.BlockSpec(memory_space=pltpu.VMEM),
        out_shape=out,
        scratch_shapes=[pltpu.VMEM((chips, total, width), LOW)] * 2 + [pltpu.VMEM((far, streams, total // PARTS, width), LOW)] * 2
        + [dma(chips)] * 3 + [dma(far, streams)] * 2,
        compiler_params=pltpu.CompilerParams(collective_id=1, has_side_effects=True, vmem_limit_bytes=VMEM),
        cost_estimate=pl.CostEstimate(flops=50_000_000_000, transcendentals=0, bytes_accessed=g.size * 2),
        name="reduce",
    )(g)


def solution(mesh):
    n = mesh.shape["dp"]

    def scatter(g):
        return lax.psum_scatter(g.reshape(-1, g.shape[2]), "dp", scatter_dimension=0, tiled=True)

    def step(x, dy, *arrays):
        weights, m, v = (arrays[i : i + 7] for i in (0, 7, 14))
        wq, wk, wv, wo, wg, wu, wd = weights
        h0, t = x[0], x.shape[1]
        half = HEAD // 2
        angle = jnp.arange(t, dtype=F32)[:, None] * THETA ** (-jnp.arange(half, dtype=F32) / half)
        cos, sin = jnp.cos(angle), jnp.sin(angle)
        me = lax.axis_index("dp").astype(jnp.int32).reshape(1)
        q0, k0, v0 = first(h0, wq, wk, wv, cos, sin, 0)
        c0, l0 = attention(q0, k0, v0)
        h1, q1, k1, v1 = middle(c0, h0, wo, wg, wu, wd, wq, wk, wv, cos, sin, 0)
        c1, l1 = attention(q1, k1, v1)
        by, by_c, g1 = mlp_back(c1, h1, dy[0], wo, wg, wu, wd, 1, n)
        dq, dk, dv = attention_back(q1, k1, v1, by_c, c1, l1)
        by, g1 = qkv_back(g1, dq, dk, dv, h1, cos, sin, 1, by, wq, wk, wv)
        r1 = scatter(g1)
        by, by_c, g0 = mlp_back(c0, h0, by, wo, wg, wu, wd, 0, n)
        dq, dk, dv = attention_back(q0, k0, v0, by_c, c0, l0)
        new1, *moments = adamw(me, r1, weights, m, v, 1, after=(dq,))
        all1 = lax.all_gather(new1, "dp", axis=0, tiled=True)
        (g0,) = qkv_back(g0, dq, dk, dv, h0, cos, sin, 0, after=[new1])
        r0 = reduce(g0)
        new0, *moments = adamw(me, r0, weights, m, v, 0, moments)
        all0 = lax.all_gather(new0, "dp", axis=0, tiled=True)
        new = unpack(all0, weights, n, 0, unpack(all1, weights, n, 1))
        return (*new, *moments)

    states, all_of, cut = P(("rep", "dp"), None, None), P(None, None, None), P(None, "dp", None)
    return jax.shard_map(
        step,
        mesh=mesh,
        in_specs=(states, states) + (all_of,) * 7 + (cut,) * 14,
        out_specs=(P("rep", None, None),) * 7 + (P("rep", "dp", None),) * 14,
        check_vma=False,
    )
```

```python
import functools

import jax
import jax.numpy as jnp
from jax import lax
from jax.experimental import pallas as pl
from jax.experimental.pallas import tpu as pltpu
from jax.sharding import PartitionSpec as P

HEAD = 256
THETA = 10000
EPS = 1e-6
HIDDEN = -2e30
LOG2E = 1.4426950408889634
LN2 = 0.6931471805599453
VMEM = 62 * 2**20
STRIP = 512
ROWS = 512
LOW = jnp.bfloat16
F32 = jnp.float32
LATE = tuple((i, 1) for i in (3, 4, 5, 6))
EARLY = tuple((i, 0) for i in (3, 4, 5, 6, 0, 1, 2)) + tuple((i, 1) for i in (0, 1, 2))


def dot(a, b, ca=1, cb=0):
    return lax.dot_general(a, b, (((ca,), (cb,)), ((), ())), preferred_element_type=F32)


def params(*semantics, **more):
    return pltpu.CompilerParams(dimension_semantics=semantics, vmem_limit_bytes=VMEM, **more)


def cost(flops, *arrays):
    return pl.CostEstimate(flops=int(flops), transcendentals=0, bytes_accessed=sum(a.size * a.dtype.itemsize for a in arrays))


def spread(h):
    wide = h.astype(F32)
    return wide, lax.rsqrt(jnp.mean(wide * wide, -1, keepdims=True) + EPS)


def norm_back(wide, scale, by):
    return scale * by - wide * (scale * scale * scale * jnp.mean(by * wide, -1, keepdims=True))


def turn(t, cos, sin):
    half, out = HEAD // 2, []
    for at in range(0, t.shape[1], HEAD):
        a, b = t[:, at : at + half].astype(F32), t[:, at + half : at + HEAD].astype(F32)
        out += [a * cos - b * sin, b * cos + a * sin]
    return jnp.concatenate(out, -1).astype(LOW)


def queries_keys_values(h, wq, wk, wv, cos, sin, q_ref, k_ref, v_ref):
    wide, scale = spread(h)
    a = (wide * scale).astype(LOW)
    q_ref[...] = turn(dot(a, wq[0]).astype(LOW), cos[...], sin[...])
    k_ref[...] = turn(dot(a, wk[0]).astype(LOW), cos[...], sin[...])
    v_ref[...] = dot(a, wv[0]).astype(LOW)


def matrix(w, layer):
    return pl.BlockSpec((1,) + w.shape[1:], lambda *_: (layer, 0, 0), pipeline_mode=pl.Buffered(1))


def rows(width, at=ROWS):
    return pl.BlockSpec((at, width), lambda i: (i, 0))


def first_kernel(h, wq, wk, wv, cos, sin, q_ref, k_ref, v_ref):
    queries_keys_values(h[...], wq, wk, wv, cos, sin, q_ref, k_ref, v_ref)


def first(h, wq, wk, wv, cos, sin, layer):
    t, d = h.shape
    n = wq.shape[2]
    outs = [jax.ShapeDtypeStruct((t, n), LOW)] * 3
    return pl.pallas_call(
        first_kernel,
        grid=(t // ROWS,),
        in_specs=[rows(d), matrix(wq, layer), matrix(wk, layer), matrix(wv, layer), rows(HEAD // 2), rows(HEAD // 2)],
        out_specs=[rows(n)] * 3,
        out_shape=outs,
        compiler_params=params("arbitrary"),
        cost_estimate=cost(6 * t * d * n, h, *outs),
        name="qkv",
    )(h, wq, wk, wv, cos, sin)


def mlp_chunk(b, wg, wu, at, size):
    gate = dot(b, wg[0, :, at : at + size])
    up = dot(b, wu[0, :, at : at + size])
    return gate, up, 0.5 * jnp.tanh(0.5 * gate) + 0.5


def middle_kernel(ctx, h, wo, wg, wu, wd, wq, wk, wv, cos, sin, out_ref, q_ref, k_ref, v_ref):
    h1 = (h[...].astype(F32) + dot(ctx[...], wo[0]).astype(LOW).astype(F32)).astype(LOW)
    wide, scale = spread(h1)
    b = (wide * scale).astype(LOW)
    ff, size = wg.shape[2], 512
    acts = []
    for at in range(0, ff, size):
        gate, up, s = mlp_chunk(b, wg, wu, at, size)
        acts.append((gate * s * up).astype(LOW))
    down = dot(jnp.concatenate(acts, -1), wd[0])
    h2 = (wide + down.astype(LOW).astype(F32)).astype(LOW)
    out_ref[...] = h2
    queries_keys_values(h2, wq, wk, wv, cos, sin, q_ref, k_ref, v_ref)


def middle(ctx, h, wo, wg, wu, wd, wq, wk, wv, cos, sin, layer):
    t, d = h.shape
    n, ff = wq.shape[2], wg.shape[2]
    outs = [jax.ShapeDtypeStruct((t, d), LOW)] + [jax.ShapeDtypeStruct((t, n), LOW)] * 3
    return pl.pallas_call(
        middle_kernel,
        grid=(t // ROWS,),
        in_specs=[rows(n), rows(d)] + [matrix(w, layer) for w in (wo, wg, wu, wd)] + [matrix(w, layer + 1) for w in (wq, wk, wv)]
        + [rows(HEAD // 2)] * 2,
        out_specs=[rows(d)] + [rows(n)] * 3,
        out_shape=outs,
        compiler_params=params("arbitrary"),
        cost_estimate=cost(2 * t * d * (4 * n + 3 * ff), h, h, *outs),
        name="middle",
    )(ctx, h, wo, wg, wu, wd, wq, wk, wv, cos, sin)


def causal_mask(size):
    return lax.broadcasted_iota(jnp.int32, (size, size), 1) >= lax.broadcasted_iota(jnp.int32, (size, size), 0)


def attention_kernel(q_ref, k_ref, v_ref, o_ref, lse_ref, mix_s, top_s):
    t, d = q_ref.shape
    e = d**-0.5 * LOG2E
    ones = jnp.ones((8, STRIP), LOW)
    blocks = [pl.ds(at, STRIP) for at in range(0, t, STRIP)]
    for j, keys in enumerate(blocks):
        k = k_ref[keys, :]
        values = jnp.concatenate([v_ref[keys, :].T, ones], axis=0)
        seen = blocks[j:]
        scores = [dot(k, q_ref[qs, :], 1, 1) for qs in seen]
        weights, keeps = [], []
        for qs, s in zip(seen, scores):
            if qs is keys:
                s = jnp.where(causal_mask(STRIP), s, HIDDEN)
            top = s.max(axis=0, keepdims=True)
            if j:
                old = top_s[0:1, qs]
                top = jnp.maximum(old, top)
                keeps.append(jnp.exp2((old - top) * e))
            top_s[0:1, qs] = top
            weights.append(jnp.exp2((s - top) * e).astype(LOW))
        for n, (qs, p) in enumerate(zip(seen, weights)):
            new = dot(values, p, 1, 0)
            if j:
                new = mix_s[:, qs] * keeps[n] + new
            if qs is keys:
                total = new[d : d + 1, :]
                o_ref[qs, :] = (new[:d, :] * (1 / total)).T.astype(LOW)
                lse_ref[0, :, qs] = top_s[0:1, qs] * e + jnp.log(total) * LOG2E
            else:
                mix_s[:, qs] = new


def head_specs(t, count):
    return [pl.BlockSpec((t, HEAD), lambda i: (0, i))] * count


def attention(q, k, v):
    t, n = q.shape
    outs = [jax.ShapeDtypeStruct((t, n), LOW), jax.ShapeDtypeStruct((n // HEAD, 1, t), F32)]
    return pl.pallas_call(
        attention_kernel,
        grid=(n // HEAD,),
        in_specs=head_specs(t, 3),
        out_specs=[*head_specs(t, 1), pl.BlockSpec((1, 1, t), lambda i: (i, 0, 0))],
        out_shape=outs,
        scratch_shapes=[pltpu.VMEM((HEAD + 8, t), F32), pltpu.VMEM((8, t), F32)],
        compiler_params=params("arbitrary"),
        cost_estimate=cost(2.5 * t * t * n, q, k, v, *outs),
        name="attention",
    )(q, k, v)


def attention_back_kernel(q_ref, k_ref, v_ref, do_ref, o_ref, lse_ref, *rest):
    dq_ref, dk_ref, dv_ref, dq_s = rest[-4:]
    t, d = q_ref.shape
    scale = d**-0.5
    e = scale * LOG2E
    blocks = [pl.ds(at, STRIP) for at in range(0, t, STRIP)]
    deltas = []
    for qs in blocks:
        both = do_ref[qs, :].astype(F32) * o_ref[qs, :].astype(F32)
        folded = sum(both[:, at : at + 128] for at in range(0, d, 128))
        deltas.append(folded.T.sum(axis=0, keepdims=True))
    for j, keys in enumerate(blocks):
        k, v = k_ref[keys, :], v_ref[keys, :]
        kt = k.T
        seen = list(enumerate(blocks))[j:]
        scores = [dot(k, q_ref[qs, :], 1, 1) for _, qs in seen]
        dps = [dot(v, do_ref[qs, :], 1, 1) for _, qs in seen]
        ps, dss = [], []
        for m, (n, qs) in enumerate(seen):
            p = jnp.exp2(scores[m] * e - lse_ref[0, :, qs])
            if n == j:
                p = jnp.where(causal_mask(STRIP), p, 0.0)
            ds = (p * (dps[m] - deltas[n])).astype(LOW)
            ps.append(p.astype(LOW))
            dss.append(ds)
            new = dot(kt, ds, 1, 0)
            if j:
                new = dq_s[:, qs] + new
            if n == j:
                dq_ref[qs, :] = (new * scale).T.astype(LOW)
            else:
                dq_s[:, qs] = new
        late = pl.ds(j * STRIP, t - j * STRIP)
        dv_ref[keys, :] = dot(jnp.concatenate(ps, axis=1), do_ref[late, :], 1, 0).astype(LOW)
        dk_ref[keys, :] = (dot(jnp.concatenate(dss, axis=1), q_ref[late, :], 1, 0) * scale).astype(LOW)


def attention_back(q, k, v, by, out, lse, after=()):
    t, n = q.shape
    outs = [jax.ShapeDtypeStruct((t, n), LOW)] * 3
    return pl.pallas_call(
        attention_back_kernel,
        grid=(n // HEAD,),
        in_specs=[*head_specs(t, 5), pl.BlockSpec((1, 1, t), lambda i: (i, 0, 0))] + [pl.BlockSpec(memory_space=pl.ANY)] * len(after),
        out_specs=head_specs(t, 3),
        out_shape=outs,
        scratch_shapes=[pltpu.VMEM((HEAD, t), F32)],
        compiler_params=params("arbitrary"),
        cost_estimate=cost(6.25 * t * t * n, q, k, v, by, out, *outs),
        name="attention_back",
    )(q, k, v, by, out, lse, *after)


def mlp_back_kernel(ctx, h, by, wo, wg, wu, wd, by_h1, by_ctx, grads, acc_o, acc_g, acc_u, acc_d):
    step = pl.program_id(0)

    @pl.when(step == 0)
    def _():
        for acc in (acc_o, acc_g, acc_u, acc_d):
            acc[...] = jnp.zeros_like(acc)

    h1 = (h[...].astype(F32) + dot(ctx[...], wo[0]).astype(LOW).astype(F32)).astype(LOW)
    wide, scale = spread(h1)
    b = (wide * scale).astype(LOW)
    bt, dyt = b.T, by[...].T
    ff, size = wg.shape[2], 512
    by_b = jnp.zeros(wide.shape, F32)
    for at in range(0, ff, size):
        here = pl.ds(at, size)
        gate, up, s = mlp_chunk(b, wg, wu, at, size)
        by_act = dot(by[...], wd[0, here, :], 1, 1).astype(LOW).astype(F32)
        silu = gate * s
        act = (silu * up).astype(LOW)
        by_up = (by_act * silu).astype(LOW)
        by_gate = (by_act * up * (s + silu * (1.0 - s))).astype(LOW)
        by_b = by_b + dot(by_gate, wg[0, :, here], 1, 1) + dot(by_up, wu[0, :, here], 1, 1)
        acc_d[:, here] += dot(dyt, act)
        acc_g[:, here] += dot(bt, by_gate)
        acc_u[:, here] += dot(bt, by_up)
    total = (by[...].astype(F32) + norm_back(wide, scale, by_b.astype(LOW).astype(F32)).astype(LOW).astype(F32)).astype(LOW)
    by_h1[...] = total
    by_ctx[...] = dot(total, wo[0], 1, 1).astype(LOW)
    acc_o[...] += dot(ctx[...].T, total)

    @pl.when(step == pl.num_programs(0) - 1)
    def _():
        n, at = grads.shape[0], 0
        for acc in (acc_o, acc_g, acc_u):
            r = acc.shape[0] // n
            for c in range(0, acc.shape[1], 512):
                grads[:, at : at + r, :] = acc[:, c : c + 512].reshape(n, r, 512).astype(LOW)
                at += r
        r = ff // n
        for first_owner in range(0, n, max(512 // r, 1)):
            many = max(512 // r, 1) if n >= max(512 // r, 1) else n
            piece = acc_d[:, first_owner * r : (first_owner + many) * r].T
            grads[first_owner : first_owner + many, at : at + r, :] = piece.reshape(many, r, 512).astype(LOW)


def mlp_back(ctx, h, by, wo, wg, wu, wd, layer, n, room=0, size=512):
    t, d = h.shape
    heads, ff = wo.shape[1], wg.shape[2]
    packed = (heads * d + 3 * d * ff) // (512 * n)
    outs = [jax.ShapeDtypeStruct((t, d), LOW), jax.ShapeDtypeStruct((t, heads), LOW), jax.ShapeDtypeStruct((n, packed + room, 512), LOW)]
    return pl.pallas_call(
        mlp_back_kernel,
        grid=(t // size,),
        in_specs=[rows(heads, size), rows(d, size), rows(d, size)] + [matrix(w, layer) for w in (wo, wg, wu, wd)],
        out_specs=[rows(d, size), rows(heads, size), pl.BlockSpec((n, packed, 512), lambda i: (0, 0, 0), pipeline_mode=pl.Buffered(1))],
        out_shape=outs,
        scratch_shapes=[pltpu.VMEM((heads, d), F32)] + [pltpu.VMEM((d, ff), F32)] * 3,
        compiler_params=params("arbitrary"),
        cost_estimate=cost(2 * t * d * (8 * ff + 3 * heads), h, h, h, *outs),
        name="mlp_back",
    )(ctx, h, by, wo, wg, wu, wd)


def qkv_back_kernel(dq, dk, dv, h, cos, sin, *rest, deeper):
    if deeper:
        by_h1, wq, wk, wv, by_h, grads, acc_q, acc_k, acc_v = rest
    else:
        packed, late, grads, acc_q, acc_k, acc_v, mine, sem = rest
    step = pl.program_id(0)

    @pl.when(step == 0)
    def _():
        for acc in (acc_q, acc_k, acc_v):
            acc[...] = jnp.zeros_like(acc)

    wide, scale = spread(h[...])
    at = (wide * scale).astype(LOW).T
    by_q, by_k = turn(dq[...], cos[...], -sin[...]), turn(dk[...], cos[...], -sin[...])
    acc_q[...] += dot(at, by_q)
    acc_k[...] += dot(at, by_k)
    acc_v[...] += dot(at, dv[...])
    if deeper:
        by_a = dot(by_q, wq[0], 1, 1) + dot(by_k, wk[0], 1, 1) + dot(dv[...], wv[0], 1, 1)
        by_h[...] = (by_h1[...].astype(F32) + norm_back(wide, scale, by_a.astype(LOW).astype(F32)).astype(LOW).astype(F32)).astype(LOW)

    @pl.when(step == pl.num_programs(0) - 1)
    def _():
        n = grads.shape[0]
        r = acc_q.shape[0] // n
        to = grads if deeper else mine
        for i, acc in enumerate((acc_q, acc_k, acc_v)):
            to[:, i * r : (i + 1) * r, :] = acc[...].reshape(n, r, 512).astype(LOW)
        if not deeper:
            mine[:, 3 * r :, :] = late[...]
            rows_here = mine.shape[1]
            copy = pltpu.make_async_copy(mine, grads.at[:, pl.ds(grads.shape[1] - rows_here, rows_here), :], sem)
            copy.start()
            copy.wait()


def qkv_back(dq, dk, dv, h, cos, sin, n, layer, by_h1=None, wq=None, wk=None, wv=None, packed=None, late=None):
    t, d = h.shape
    heads = dq.shape[1]
    deeper = packed is None
    whole = pl.BlockSpec((n, 3 * d // n, heads), lambda i: (0, 0, 0), pipeline_mode=pl.Buffered(1))
    anywhere = pl.BlockSpec(memory_space=pl.ANY)
    given, specs = [dq, dk, dv, h, cos, sin], [rows(heads)] * 3 + [rows(d)] + [rows(HEAD // 2)] * 2
    scratch = [pltpu.VMEM((d, heads), F32)] * 3
    if deeper:
        given += [by_h1, wq, wk, wv]
        specs += [rows(d)] + [matrix(w, layer) for w in (wq, wk, wv)]
        outs = [jax.ShapeDtypeStruct((t, d), LOW), jax.ShapeDtypeStruct((n, 3 * d // n, heads), LOW)]
        out_specs = [rows(d), whole]
    else:
        given += [packed, late]
        specs += [anywhere, whole]
        outs, out_specs = [jax.ShapeDtypeStruct(packed.shape, LOW)], [anywhere]
        scratch += [pltpu.VMEM((n, 6 * d // n, heads), LOW), pltpu.SemaphoreType.DMA]
    return pl.pallas_call(
        functools.partial(qkv_back_kernel, deeper=deeper),
        grid=(t // ROWS,),
        in_specs=specs,
        out_specs=out_specs,
        out_shape=outs,
        scratch_shapes=scratch,
        input_output_aliases={} if deeper else {6: 0},
        compiler_params=params("arbitrary"),
        cost_estimate=cost(2 * t * d * heads * (6 if deeper else 3), dq, dk, dv, h, h, h),
        name="qkv_back",
    )(*given)


def layers_of(plan):
    return {i: [layer for j, layer in plan if j == i] for i in sorted({i for i, _ in plan})}


def adamw_kernel(me, packed_g, *refs, plan):
    used = layers_of(plan)
    count = len(used)
    ws, ms, vs = (dict(zip(used, refs[k * count : (k + 1) * count])) for k in range(3))
    rest = refs[-1 - 2 * count :]
    packed, new_m, new_v = rest[0], dict(zip(used, rest[1 : 1 + count])), dict(zip(used, rest[1 + count :]))
    at = 0
    for i, layer in plan:
        x = layer - used[i][0]
        r, width = ms[i].shape[1], ms[i].shape[2]
        for c in range(0, width, 512):
            cols = slice(c, c + 512)
            g = packed_g[at : at + r, :].astype(F32)
            m = 0.9 * ms[i][x, :, cols] + 0.1 * g
            v = 0.95 * vs[i][x, :, cols] + 0.05 * g * g
            w = ws[i][x, :, cols].astype(F32)
            new_m[i][x, :, cols] = m
            new_v[i][x, :, cols] = v
            packed[at : at + r, :] = (w - 0.02 * (m * lax.rsqrt(v + 1e-8) + 0.1 * w)).astype(LOW)
            at += r


def adamw(me, g, ws, ms, vs, plan, earlier=None, after=()):
    used, earlier = layers_of(plan), earlier or {}
    spec = lambda i, mine: pl.BlockSpec((len(used[i]),) + ms[i].shape[1:], lambda _, me: (used[i][0], me[0] if mine else 0, 0))
    own, part = [spec(i, True) for i in used], [spec(i, False) for i in used]
    total = g.shape[0]
    outs = [jax.ShapeDtypeStruct((total, 512), LOW)] + [jax.ShapeDtypeStruct(ms[i].shape, F32) for _ in range(2) for i in used]
    known = [earlier[i][k] for k in range(2) for i in earlier]
    given = [g] + [a[i] for a in (ws, ms, vs) for i in used] + known + list(after)
    first = 2 + 3 * len(used)
    to = [1 + k * len(used) + list(used).index(i) for k in range(2) for i in earlier]
    new, *moments = pl.pallas_call(
        functools.partial(adamw_kernel, plan=plan),
        grid_spec=pltpu.PrefetchScalarGridSpec(
            num_scalar_prefetch=1,
            grid=(1,),
            in_specs=[pl.BlockSpec(g.shape, lambda _, me: (0, 0)), *own, *part, *part] + [pl.BlockSpec(memory_space=pl.ANY)] * len([*known, *after]),
            out_specs=[pl.BlockSpec((total, 512), lambda _, me: (0, 0)), *part, *part],
        ),
        out_shape=outs,
        input_output_aliases={first + i: o for i, o in enumerate(to)},
        compiler_params=params("arbitrary"),
        cost_estimate=cost(20 * total * 512, g, *outs),
        name="adamw",
    )(me, *given)
    return new, {i: (moments[x], moments[x + len(used)]) for x, i in enumerate(used)}


def unpack_kernel(packed, *refs, plan):
    used = layers_of(plan)
    outs, at = dict(zip(used, refs[-len(used) :])), 0
    owners = packed.shape[0]
    for i, layer in plan:
        out = outs[i]
        r = out.shape[1] // owners
        for c in range(0, out.shape[2], 512):
            for owner in range(owners):
                out[layer - used[i][0], owner * r : (owner + 1) * r, c : c + 512] = packed[owner, at : at + r, :]
            at += r


def unpack(packed, ws, n, plan, earlier=None):
    used, earlier = layers_of(plan), earlier or {}
    outs = [jax.ShapeDtypeStruct(ws[i].shape, LOW) for i in used]
    total = packed.shape[0] // n
    some = min(n, 4)
    new = pl.pallas_call(
        functools.partial(unpack_kernel, plan=plan),
        grid=(n // some,),
        in_specs=[pl.BlockSpec((some, total, 512), lambda i: (i, 0, 0))] + [pl.BlockSpec(memory_space=pl.ANY)] * len(earlier),
        out_specs=[pl.BlockSpec((len(used[i]), some * ws[i].shape[1] // n, ws[i].shape[2]), lambda at, i=i: (used[i][0], at, 0)) for i in used],
        out_shape=outs,
        input_output_aliases={1 + x: list(used).index(i) for x, i in enumerate(earlier)},
        compiler_params=params("arbitrary"),
        cost_estimate=cost(0, *outs),
        name="unpack",
    )(packed.reshape(n, total, 512), *earlier.values())
    return dict(zip(used, new))


CORES = 2
PARTS = 4


def part_rows(total):
    long = -(-total // (2 * 16 * 2)) * 16
    short = total // 2 - long
    return (0, long), (long, short), (total // 2, long), (total // 2 + long, short)


def reduce_kernel(g, out, mine, pair, sent, got, mine_sem, pair_send, pair_got, send_sem, got_sem):
    n, total = g.shape[0], g.shape[1]
    chips = n // CORES
    far, parts = chips // 2, part_rows(total)
    me = lax.axis_index("dp")
    z, core = lax.div(me, CORES), lax.rem(me, CORES)
    at = lambda chip, which: {"dp": lax.rem(chip + chips, chips) * CORES + which}
    peers = {1: at(z + 1, core), -1: at(z - 1, core)}
    partner = at(z, 1 - core)

    barrier = pltpu.get_barrier_semaphore()
    for peer in (peers[1], peers[-1], partner):
        pl.semaphore_signal(barrier, inc=1, device_id=peer, device_id_type=pl.DeviceIdType.MESH)

    order = [far] + [x * sign for x in range(far - 1, 0, -1) for sign in (1, -1)] + [0]
    slot = {offset: i for i, offset in enumerate(order)} | {-far: 0}
    local = []
    for i, offset in enumerate(order):
        chunk = lax.rem(z + offset + chips, chips) * CORES
        local.append(pltpu.make_async_copy(g.at[chunk + core], mine.at[i], mine_sem.at[i]))
        local[i].start()
    pl.semaphore_wait(barrier, 3)
    across = []
    for i, offset in enumerate(order):
        chunk = lax.rem(z + offset + chips, chips) * CORES
        across.append(pltpu.make_async_remote_copy(g.at[chunk + 1 - core], pair.at[i], pair_send.at[i], pair_got.at[i], device_id=partner,
                                                   device_id_type=pl.DeviceIdType.MESH))
        across[i].start()

    streams = [(sign, part, far if (part < PARTS // 2) == (sign > 0) else far - 1) for part in range(PARTS) for sign in (1, -1)]
    ready, copies = set(), {}

    def own(offset, here):
        i = slot[offset]
        if i not in ready:
            ready.add(i)
            local[i].wait()
            across[i].wait_recv()
        return mine[i, here, :].astype(F32) + pair[i, here, :].astype(F32)

    for s in range(far):
        pending = None
        for x, (sign, part, hops) in enumerate(streams):
            if s < hops:
                value = own(sign * (hops - s), pl.ds(*parts[part]))
                if s:
                    copies[s - 1, x].wait_recv()
                    value = value + got[s - 1, x, : parts[part][1]].astype(F32)
                many = pl.ds(0, parts[part][1])
                sent[s, x, many] = value.astype(LOW)
                copies[s, x] = pltpu.make_async_remote_copy(sent.at[s, x, many], got.at[s, x, many], send_sem.at[s, x], got_sem.at[s, x],
                                                            device_id=peers[sign], device_id_type=pl.DeviceIdType.MESH)
                if pending is not None:
                    pending.start()
                pending = copies[s, x]
        pending.start()
    for part in range(PARTS):
        here = pl.ds(*parts[part])
        value = own(0, here)
        for x, (_, of, hops) in enumerate(streams):
            if of == part:
                copies[hops - 1, x].wait_recv()
                value = value + got[hops - 1, x, : parts[part][1]].astype(F32)
        out[here, :] = value.astype(LOW)
    for copy in (*across, *copies.values()):
        copy.wait_send()


def reduce(g):
    n, total, width = g.shape
    chips = n // CORES
    far, streams = chips // 2, 2 * PARTS
    out = jax.ShapeDtypeStruct((total, width), LOW)
    dma = lambda *shape: pltpu.SemaphoreType.DMA(shape)
    return pl.pallas_call(
        reduce_kernel,
        in_specs=[pl.BlockSpec(memory_space=pl.ANY)],
        out_specs=pl.BlockSpec(memory_space=pltpu.VMEM),
        out_shape=out,
        scratch_shapes=[pltpu.VMEM((chips, total, width), LOW)] * 2 + [pltpu.VMEM((far, streams, part_rows(total)[0][1], width), LOW)] * 2
        + [dma(chips)] * 3 + [dma(far, streams)] * 2,
        compiler_params=pltpu.CompilerParams(collective_id=1, has_side_effects=True, vmem_limit_bytes=VMEM),
        cost_estimate=pl.CostEstimate(flops=50_000_000_000, transcendentals=0, bytes_accessed=g.size * 2),
        name="reduce",
    )(g)


def solution(mesh):
    n = mesh.shape["dp"]

    def scatter(g):
        return lax.psum_scatter(g.reshape(-1, g.shape[2]), "dp", scatter_dimension=0, tiled=True)

    def step(x, dy, *arrays):
        weights, m, v = (arrays[i : i + 7] for i in (0, 7, 14))
        wq, wk, wv, wo, wg, wu, wd = weights
        h0, t = x[0], x.shape[1]
        half = HEAD // 2
        angle = jnp.arange(t, dtype=F32)[:, None] * THETA ** (-jnp.arange(half, dtype=F32) / half)
        cos, sin = jnp.cos(angle), jnp.sin(angle)
        me = lax.axis_index("dp").astype(jnp.int32).reshape(1)
        q0, k0, v0 = first(h0, wq, wk, wv, cos, sin, 0)
        c0, l0 = attention(q0, k0, v0)
        h1, q1, k1, v1 = middle(c0, h0, wo, wg, wu, wd, wq, wk, wv, cos, sin, 0)
        c1, l1 = attention(q1, k1, v1)
        by, by_c, g1 = mlp_back(c1, h1, dy[0], wo, wg, wu, wd, 1, n)
        r1 = scatter(g1)
        dq, dk, dv = attention_back(q1, k1, v1, by_c, c1, l1)
        by, late = qkv_back(dq, dk, dv, h1, cos, sin, n, 1, by, wq, wk, wv)
        by, by_c, g0 = mlp_back(c0, h0, by, wo, wg, wu, wd, 0, n, 2 * late.shape[1])
        new1, moments = adamw(me, r1, weights, m, v, LATE, after=(by_c,))
        all1 = lax.all_gather(new1, "dp", axis=0, tiled=True)
        dq, dk, dv = attention_back(q0, k0, v0, by_c, c0, l0, after=(new1,))
        (g0,) = qkv_back(dq, dk, dv, h0, cos, sin, n, 0, packed=g0, late=late)
        new0, moments = adamw(me, reduce(g0), weights, m, v, EARLY, moments)
        all0 = lax.all_gather(new0, "dp", axis=0, tiled=True)
        new = unpack(all0, weights, n, EARLY, unpack(all1, weights, n, LATE))
        return tuple(new[i] for i in range(7)) + tuple(moments[i][which] for which in range(2) for i in range(7))

    states, all_of, cut = P(("rep", "dp"), None, None), P(None, None, None), P(None, "dp", None)
    return jax.shard_map(
        step,
        mesh=mesh,
        in_specs=(states, states) + (all_of,) * 7 + (cut,) * 14,
        out_specs=(P("rep", None, None),) * 7 + (P("rep", "dp", None),) * 14,
        check_vma=False,
    )
```

```python
import functools

import jax
import jax.numpy as jnp
from jax import lax
from jax.experimental import pallas as pl
from jax.experimental.pallas import tpu as pltpu
from jax.sharding import PartitionSpec as P

HEAD = 256
THETA = 10000
EPS = 1e-6
HIDDEN = -2e30
LOG2E = 1.4426950408889634
LN2 = 0.6931471805599453
VMEM = 62 * 2**20
STRIP = 512
ROWS = 512
LOW = jnp.bfloat16
F32 = jnp.float32
LATE = tuple((i, 1) for i in (3, 4, 5, 6))
EARLY = tuple((i, 0) for i in (3, 4, 5, 6, 0, 1, 2)) + tuple((i, 1) for i in (0, 1, 2))


def dot(a, b, ca=1, cb=0):
    return lax.dot_general(a, b, (((ca,), (cb,)), ((), ())), preferred_element_type=F32)


def params(*semantics, **more):
    return pltpu.CompilerParams(dimension_semantics=semantics, vmem_limit_bytes=VMEM, **more)


def cost(flops, *arrays):
    return pl.CostEstimate(flops=int(flops), transcendentals=0, bytes_accessed=sum(a.size * a.dtype.itemsize for a in arrays))


def spread(h):
    wide = h.astype(F32)
    return wide, lax.rsqrt(jnp.mean(wide * wide, -1, keepdims=True) + EPS)


def norm_back(wide, scale, by):
    return scale * by - wide * (scale * scale * scale * jnp.mean(by * wide, -1, keepdims=True))


def turn(t, cos, sin):
    half, out = HEAD // 2, []
    for at in range(0, t.shape[1], HEAD):
        a, b = t[:, at : at + half].astype(F32), t[:, at + half : at + HEAD].astype(F32)
        out += [a * cos - b * sin, b * cos + a * sin]
    return jnp.concatenate(out, -1).astype(LOW)


def queries_keys_values(h, wq, wk, wv, cos, sin, q_ref, k_ref, v_ref):
    wide, scale = spread(h)
    a = (wide * scale).astype(LOW)
    q_ref[...] = turn(dot(a, wq[0]).astype(LOW), cos[...], sin[...])
    k_ref[...] = turn(dot(a, wk[0]).astype(LOW), cos[...], sin[...])
    v_ref[...] = dot(a, wv[0]).astype(LOW)


def matrix(w, layer):
    return pl.BlockSpec((1,) + w.shape[1:], lambda *_: (layer, 0, 0), pipeline_mode=pl.Buffered(1))


def rows(width, at=ROWS):
    return pl.BlockSpec((at, width), lambda i: (i, 0))


def first_kernel(h, wq, wk, wv, cos, sin, q_ref, k_ref, v_ref):
    queries_keys_values(h[...], wq, wk, wv, cos, sin, q_ref, k_ref, v_ref)


def first(h, wq, wk, wv, cos, sin, layer):
    t, d = h.shape
    n = wq.shape[2]
    outs = [jax.ShapeDtypeStruct((t, n), LOW)] * 3
    return pl.pallas_call(
        first_kernel,
        grid=(t // ROWS,),
        in_specs=[rows(d), matrix(wq, layer), matrix(wk, layer), matrix(wv, layer), rows(HEAD // 2), rows(HEAD // 2)],
        out_specs=[rows(n)] * 3,
        out_shape=outs,
        compiler_params=params("arbitrary"),
        cost_estimate=cost(6 * t * d * n, h, *outs),
        name="qkv",
    )(h, wq, wk, wv, cos, sin)


def mlp_chunk(b, wg, wu, at, size):
    gate = dot(b, wg[0, :, at : at + size])
    up = dot(b, wu[0, :, at : at + size])
    return gate, up, 0.5 * jnp.tanh(0.5 * gate) + 0.5


def middle_kernel(ctx, h, wo, wg, wu, wd, wq, wk, wv, cos, sin, out_ref, q_ref, k_ref, v_ref):
    h1 = (h[...].astype(F32) + dot(ctx[...], wo[0]).astype(LOW).astype(F32)).astype(LOW)
    wide, scale = spread(h1)
    b = (wide * scale).astype(LOW)
    ff, size = wg.shape[2], 512
    acts = []
    for at in range(0, ff, size):
        gate, up, s = mlp_chunk(b, wg, wu, at, size)
        acts.append((gate * s * up).astype(LOW))
    down = dot(jnp.concatenate(acts, -1), wd[0])
    h2 = (wide + down.astype(LOW).astype(F32)).astype(LOW)
    out_ref[...] = h2
    queries_keys_values(h2, wq, wk, wv, cos, sin, q_ref, k_ref, v_ref)


def middle(ctx, h, wo, wg, wu, wd, wq, wk, wv, cos, sin, layer):
    t, d = h.shape
    n, ff = wq.shape[2], wg.shape[2]
    outs = [jax.ShapeDtypeStruct((t, d), LOW)] + [jax.ShapeDtypeStruct((t, n), LOW)] * 3
    return pl.pallas_call(
        middle_kernel,
        grid=(t // ROWS,),
        in_specs=[rows(n), rows(d)] + [matrix(w, layer) for w in (wo, wg, wu, wd)] + [matrix(w, layer + 1) for w in (wq, wk, wv)]
        + [rows(HEAD // 2)] * 2,
        out_specs=[rows(d)] + [rows(n)] * 3,
        out_shape=outs,
        compiler_params=params("arbitrary"),
        cost_estimate=cost(2 * t * d * (4 * n + 3 * ff), h, h, *outs),
        name="middle",
    )(ctx, h, wo, wg, wu, wd, wq, wk, wv, cos, sin)


def causal_mask(size):
    return lax.broadcasted_iota(jnp.int32, (size, size), 1) >= lax.broadcasted_iota(jnp.int32, (size, size), 0)


def attention_kernel(q_ref, k_ref, v_ref, o_ref, lse_ref, mix_s, top_s):
    t, d = q_ref.shape
    e = d**-0.5 * LOG2E
    ones = jnp.ones((8, STRIP), LOW)
    blocks = [pl.ds(at, STRIP) for at in range(0, t, STRIP)]
    for j, keys in enumerate(blocks):
        k = k_ref[keys, :]
        values = jnp.concatenate([v_ref[keys, :].T, ones], axis=0)
        seen = blocks[j:]
        scores = [dot(k, q_ref[qs, :], 1, 1) for qs in seen]
        weights, keeps = [], []
        for qs, s in zip(seen, scores):
            if qs is keys:
                s = jnp.where(causal_mask(STRIP), s, HIDDEN)
            top = s.max(axis=0, keepdims=True)
            if j:
                old = top_s[0:1, qs]
                top = jnp.maximum(old, top)
                keeps.append(jnp.exp2((old - top) * e))
            top_s[0:1, qs] = top
            weights.append(jnp.exp2((s - top) * e).astype(LOW))
        for n, (qs, p) in enumerate(zip(seen, weights)):
            new = dot(values, p, 1, 0)
            if j:
                new = mix_s[:, qs] * keeps[n] + new
            if qs is keys:
                total = new[d : d + 1, :]
                o_ref[qs, :] = (new[:d, :] * (1 / total)).T.astype(LOW)
                lse_ref[0, :, qs] = top_s[0:1, qs] * e + jnp.log(total) * LOG2E
            else:
                mix_s[:, qs] = new


def head_specs(t, count):
    return [pl.BlockSpec((t, HEAD), lambda i: (0, i))] * count


def attention(q, k, v):
    t, n = q.shape
    outs = [jax.ShapeDtypeStruct((t, n), LOW), jax.ShapeDtypeStruct((n // HEAD, 1, t), F32)]
    return pl.pallas_call(
        attention_kernel,
        grid=(n // HEAD,),
        in_specs=head_specs(t, 3),
        out_specs=[*head_specs(t, 1), pl.BlockSpec((1, 1, t), lambda i: (i, 0, 0))],
        out_shape=outs,
        scratch_shapes=[pltpu.VMEM((HEAD + 8, t), F32), pltpu.VMEM((8, t), F32)],
        compiler_params=params("arbitrary"),
        cost_estimate=cost(2.5 * t * t * n, q, k, v, *outs),
        name="attention",
    )(q, k, v)


def attention_back_kernel(q_ref, k_ref, v_ref, do_ref, o_ref, lse_ref, h, cos, sin, *rest, deeper):
    if deeper:
        by_h1, wq, wk, wv = rest[:4]
        by_h, grads, dq_s, at_s, by_q, by_k, by_v, mine, sem, by_a = rest[4:]
    else:
        late = rest[1]
        grads, dq_s, at_s, by_q, by_k, by_v, mine, sem = rest[-8:]
    t, d = q_ref.shape
    n, head = grads.shape[0], pl.program_id(0)
    scale = d**-0.5
    e = scale * LOG2E
    blocks = [pl.ds(at, STRIP) for at in range(0, t, STRIP)]

    @pl.when(head == 0)
    def _():
        for qs in blocks:
            wide, size = spread(h[qs, :])
            at_s[:, qs] = (wide * size).astype(LOW).T

    deltas = []
    for qs in blocks:
        both = do_ref[qs, :].astype(F32) * o_ref[qs, :].astype(F32)
        folded = sum(both[:, at : at + 128] for at in range(0, d, 128))
        deltas.append(folded.T.sum(axis=0, keepdims=True))
    for j, keys in enumerate(blocks):
        k, v = k_ref[keys, :], v_ref[keys, :]
        kt = k.T
        seen = list(enumerate(blocks))[j:]
        scores = [dot(k, q_ref[qs, :], 1, 1) for _, qs in seen]
        dps = [dot(v, do_ref[qs, :], 1, 1) for _, qs in seen]
        ps, dss = [], []
        for m, (x, qs) in enumerate(seen):
            p = jnp.exp2(scores[m] * e - lse_ref[0, :, qs])
            if x == j:
                p = jnp.where(causal_mask(STRIP), p, 0.0)
            ds = (p * (dps[m] - deltas[x])).astype(LOW)
            ps.append(p.astype(LOW))
            dss.append(ds)
            new = dot(kt, ds, 1, 0)
            if j:
                new = dq_s[:, qs] + new
            if x == j:
                by_q[qs, :] = turn((new * scale).T.astype(LOW), cos[qs, :], -sin[qs, :])
            else:
                dq_s[:, qs] = new
        late_q = pl.ds(j * STRIP, t - j * STRIP)
        by_v[keys, :] = dot(jnp.concatenate(ps, axis=1), do_ref[late_q, :], 1, 0).astype(LOW)
        dk = (dot(jnp.concatenate(dss, axis=1), q_ref[late_q, :], 1, 0) * scale).astype(LOW)
        by_k[keys, :] = turn(dk, cos[keys, :], -sin[keys, :])

    r = at_s.shape[0] // n
    for i, by in enumerate((by_q, by_k, by_v)):
        mine[:, i * r : (i + 1) * r, :] = dot(at_s[...], by[...]).reshape(n, r, d).astype(LOW)
    base = 0 if deeper else grads.shape[1] - 6 * r
    copies = [pltpu.make_async_copy(mine, grads.at[:, pl.ds(base, 3 * r), pl.ds(pl.multiple_of(head * d, d), d)], sem.at[0])]
    copies[0].start()
    if not deeper:
        copies.append(pltpu.make_async_copy(late, grads.at[:, pl.ds(base + 3 * r, 3 * r), :], sem.at[1]))

        @pl.when(head == 0)
        def _():
            copies[1].start()
            copies[1].wait()
    else:
        for qs in blocks:
            term = dot(by_q[qs, :], wq[0], 1, 1) + dot(by_k[qs, :], wk[0], 1, 1) + dot(by_v[qs, :], wv[0], 1, 1)
            by_a[qs, :] = jnp.where(head == 0, term, by_a[qs, :] + term)

        @pl.when(head == pl.num_programs(0) - 1)
        def _():
            for qs in blocks:
                wide, size = spread(h[qs, :])
                back = norm_back(wide, size, by_a[qs, :].astype(LOW).astype(F32)).astype(LOW).astype(F32)
                by_h[qs, :] = (by_h1[qs, :].astype(F32) + back).astype(LOW)
    copies[0].wait()


def attention_back(q, k, v, by, out, lse, h, cos, sin, n, layer, by_h1=None, wq=None, wk=None, wv=None, packed=None, late=None, after=()):
    t, width = q.shape
    d = h.shape[1]
    deeper = packed is None
    once = lambda a: pl.BlockSpec(a.shape, lambda i: (0,) * a.ndim, pipeline_mode=pl.Buffered(1))
    anywhere = pl.BlockSpec(memory_space=pl.ANY)
    given = [q, k, v, by, out, lse, h, cos, sin]
    specs = [*head_specs(t, 5), pl.BlockSpec((1, 1, t), lambda i: (i, 0, 0)), once(h), once(cos), once(sin)]
    scratch = [pltpu.VMEM((HEAD, t), F32), pltpu.VMEM((d, t), LOW)] + [pltpu.VMEM((t, HEAD), LOW)] * 3
    scratch += [pltpu.VMEM((n, 3 * d // n, HEAD), LOW), pltpu.SemaphoreType.DMA((2,))]
    if deeper:
        given += [by_h1, wq, wk, wv]
        specs += [once(by_h1)] + [pl.BlockSpec((1, d, HEAD), lambda i: (layer, 0, i))] * 3
        outs = [jax.ShapeDtypeStruct((t, d), LOW), jax.ShapeDtypeStruct((n, 3 * d // n, width), LOW)]
        out_specs = [once(h), anywhere]
        scratch += [pltpu.VMEM((t, d), F32)]
    else:
        given += [packed, late, *after]
        specs += [anywhere, once(late)] + [anywhere] * len(after)
        outs, out_specs = [jax.ShapeDtypeStruct(packed.shape, LOW)], [anywhere]
    return pl.pallas_call(
        functools.partial(attention_back_kernel, deeper=deeper),
        grid=(width // HEAD,),
        in_specs=specs,
        out_specs=out_specs,
        out_shape=outs,
        scratch_shapes=scratch,
        input_output_aliases={} if deeper else {9: 0},
        compiler_params=params("arbitrary"),
        cost_estimate=cost(6.25 * t * t * width + 2 * t * d * width * (6 if deeper else 3), q, k, v, by, out, h, h),
        name="attention_back",
    )(*given)


def mlp_back_kernel(ctx, h, by, wo, wg, wu, wd, by_h1, by_ctx, grads, acc_o, acc_g, acc_u, acc_d, b_s, bt_s, dyt_s, by_b, stage, sems):
    step = pl.program_id(0)
    last = step == pl.num_programs(0) - 1
    n, d, ff = grads.shape[0], wg.shape[1], wg.shape[2]
    r, rd, chunks = d // n, ff // n, ff // CHUNK
    many = CHUNK // rd

    def put(acc, where, term):
        acc[where] = jnp.where(step == 0, term, acc[where] + term)

    def leave(owners, first, count, i, kind):
        where = (owners, pl.ds(first, count))
        return pltpu.make_async_copy(stage.at[where], grads.at[where], sems.at[kind, i])

    def leaving(c):
        gate_rows = pl.multiple_of(r + c * r, r)
        up_rows = pl.multiple_of(r + (chunks + c) * r, r)
        owners = pl.ds(pl.multiple_of(c * many, many), many)
        return gate_rows, up_rows, owners, (leave(pl.ds(0, n), gate_rows, r, c, 0), leave(pl.ds(0, n), up_rows, r, c, 1),
                                            leave(owners, r * (1 + 2 * chunks), rd, c, 2))

    h1 = (h[...].astype(F32) + dot(ctx[...], wo[0]).astype(LOW).astype(F32)).astype(LOW)
    wide, scale = spread(h1)
    b = (wide * scale).astype(LOW)
    b_s[...] = b
    bt_s[...] = b.T
    dyt_s[...] = by[...].T
    by_b[...] = jnp.zeros(by_b.shape, F32)

    def chunk(c):
        here = pl.ds(pl.multiple_of(c * CHUNK, CHUNK), CHUNK)
        gate, up = dot(b_s[...], wg[0, :, here]), dot(b_s[...], wu[0, :, here])
        s = 0.5 * jnp.tanh(0.5 * gate) + 0.5
        by_act = dot(by[...], wd[0, here, :], 1, 1).astype(LOW).astype(F32)
        silu = gate * s
        act = (silu * up).astype(LOW)
        by_up = (by_act * silu).astype(LOW)
        by_gate = (by_act * up * (s + silu * (1.0 - s))).astype(LOW)
        by_b[...] += dot(by_gate, wg[0, :, here], 1, 1) + dot(by_up, wu[0, :, here], 1, 1)
        put(acc_d, (slice(None), here), dot(dyt_s[...], act))
        put(acc_g, (slice(None), here), dot(bt_s[...], by_gate))
        put(acc_u, (slice(None), here), dot(bt_s[...], by_up))

    def two(i, _):
        for c in (2 * i, 2 * i + 1):
            chunk(c)

        @pl.when(last)
        def _():
            for c in (2 * i, 2 * i + 1):
                here = pl.ds(pl.multiple_of(c * CHUNK, CHUNK), CHUNK)
                gate_rows, up_rows, owners, copies = leaving(c)
                stage[:, pl.ds(gate_rows, r), :] = acc_g[:, here].reshape(n, r, CHUNK).astype(LOW)
                stage[:, pl.ds(up_rows, r), :] = acc_u[:, here].reshape(n, r, CHUNK).astype(LOW)
                stage[owners, r * (1 + 2 * chunks) :, :] = acc_d[:, here].T.reshape(many, rd, d).astype(LOW)
                for copy in copies:
                    copy.start()

    lax.fori_loop(0, chunks // 2, two, None)
    wide, scale = spread(h1)
    total = (by[...].astype(F32) + norm_back(wide, scale, by_b[...].astype(LOW).astype(F32)).astype(LOW).astype(F32)).astype(LOW)
    by_h1[...] = total
    by_ctx[...] = dot(total, wo[0], 1, 1).astype(LOW)
    put(acc_o, (slice(None), slice(None)), dot(ctx[...].T, total))

    @pl.when(last)
    def _():
        stage[:, :r, :] = acc_o[...].reshape(n, r, d).astype(LOW)
        copy = leave(pl.ds(0, n), 0, r, 0, 3)
        copy.start()
        for c in range(chunks):
            for each in leaving(c)[3]:
                each.wait()
        copy.wait()


CHUNK = 512


def mlp_back(ctx, h, by, wo, wg, wu, wd, layer, n, room=0, size=512):
    t, d = h.shape
    heads, ff = wo.shape[1], wg.shape[2]
    packed = (heads * d + 3 * d * ff) // (512 * n)
    outs = [jax.ShapeDtypeStruct((t, d), LOW), jax.ShapeDtypeStruct((t, heads), LOW), jax.ShapeDtypeStruct((n, packed + room, 512), LOW)]
    return pl.pallas_call(
        mlp_back_kernel,
        grid=(t // size,),
        in_specs=[rows(heads, size), rows(d, size), rows(d, size)] + [matrix(w, layer) for w in (wo, wg, wu, wd)],
        out_specs=[rows(d, size), rows(heads, size), pl.BlockSpec(memory_space=pl.ANY)],
        out_shape=outs,
        scratch_shapes=[pltpu.VMEM((heads, d), F32)] + [pltpu.VMEM((d, ff), F32)] * 3
        + [pltpu.VMEM((size, d), LOW), pltpu.VMEM((d, size), LOW), pltpu.VMEM((d, size), LOW), pltpu.VMEM((size, d), F32)]
        + [pltpu.VMEM((n, packed, 512), LOW), pltpu.SemaphoreType.DMA((4, ff // CHUNK))],
        compiler_params=params("arbitrary"),
        cost_estimate=cost(2 * t * d * (8 * ff + 3 * heads), h, h, h, *outs),
        name="mlp_back",
    )(ctx, h, by, wo, wg, wu, wd)


def layers_of(plan):
    return {i: [layer for j, layer in plan if j == i] for i in sorted({i for i, _ in plan})}


def adamw_kernel(me, packed_g, *refs, plan):
    used = layers_of(plan)
    count = len(used)
    ws, ms, vs = (dict(zip(used, refs[k * count : (k + 1) * count])) for k in range(3))
    rest = refs[-1 - 2 * count :]
    packed, new_m, new_v = rest[0], dict(zip(used, rest[1 : 1 + count])), dict(zip(used, rest[1 + count :]))
    at = 0
    for i, layer in plan:
        x = layer - used[i][0]
        r, width = ms[i].shape[1], ms[i].shape[2]
        for c in range(0, width, 512):
            cols = slice(c, c + 512)
            g = packed_g[at : at + r, :].astype(F32)
            m = 0.9 * ms[i][x, :, cols] + 0.1 * g
            v = 0.95 * vs[i][x, :, cols] + 0.05 * g * g
            w = ws[i][x, :, cols].astype(F32)
            new_m[i][x, :, cols] = m
            new_v[i][x, :, cols] = v
            packed[at : at + r, :] = (w - 0.02 * (m * lax.rsqrt(v + 1e-8) + 0.1 * w)).astype(LOW)
            at += r


def adamw(me, g, ws, ms, vs, plan, earlier=None, after=()):
    used, earlier = layers_of(plan), earlier or {}
    spec = lambda i, mine: pl.BlockSpec((len(used[i]),) + ms[i].shape[1:], lambda _, me: (used[i][0], me[0] if mine else 0, 0))
    own, part = [spec(i, True) for i in used], [spec(i, False) for i in used]
    total = g.shape[0]
    outs = [jax.ShapeDtypeStruct((total, 512), LOW)] + [jax.ShapeDtypeStruct(ms[i].shape, F32) for _ in range(2) for i in used]
    known = [earlier[i][k] for k in range(2) for i in earlier]
    given = [g] + [a[i] for a in (ws, ms, vs) for i in used] + known + list(after)
    first = 2 + 3 * len(used)
    to = [1 + k * len(used) + list(used).index(i) for k in range(2) for i in earlier]
    new, *moments = pl.pallas_call(
        functools.partial(adamw_kernel, plan=plan),
        grid_spec=pltpu.PrefetchScalarGridSpec(
            num_scalar_prefetch=1,
            grid=(1,),
            in_specs=[pl.BlockSpec(g.shape, lambda _, me: (0, 0)), *own, *part, *part] + [pl.BlockSpec(memory_space=pl.ANY)] * len([*known, *after]),
            out_specs=[pl.BlockSpec((total, 512), lambda _, me: (0, 0)), *part, *part],
        ),
        out_shape=outs,
        input_output_aliases={first + i: o for i, o in enumerate(to)},
        compiler_params=params("arbitrary"),
        cost_estimate=cost(20 * total * 512, g, *outs),
        name="adamw",
    )(me, *given)
    return new, {i: (moments[x], moments[x + len(used)]) for x, i in enumerate(used)}


def unpack_kernel(packed, *refs, plan):
    used = layers_of(plan)
    outs, at = dict(zip(used, refs[-len(used) :])), 0
    owners = packed.shape[0]
    for i, layer in plan:
        out = outs[i]
        r = out.shape[1] // owners
        for c in range(0, out.shape[2], 512):
            for owner in range(owners):
                out[layer - used[i][0], owner * r : (owner + 1) * r, c : c + 512] = packed[owner, at : at + r, :]
            at += r


def unpack(packed, ws, n, plan, earlier=None):
    used, earlier = layers_of(plan), earlier or {}
    outs = [jax.ShapeDtypeStruct(ws[i].shape, LOW) for i in used]
    total = packed.shape[0] // n
    some = min(n, 4)
    new = pl.pallas_call(
        functools.partial(unpack_kernel, plan=plan),
        grid=(n // some,),
        in_specs=[pl.BlockSpec((some, total, 512), lambda i: (i, 0, 0))] + [pl.BlockSpec(memory_space=pl.ANY)] * len(earlier),
        out_specs=[pl.BlockSpec((len(used[i]), some * ws[i].shape[1] // n, ws[i].shape[2]), lambda at, i=i: (used[i][0], at, 0)) for i in used],
        out_shape=outs,
        input_output_aliases={1 + x: list(used).index(i) for x, i in enumerate(earlier)},
        compiler_params=params("arbitrary"),
        cost_estimate=cost(0, *outs),
        name="unpack",
    )(packed.reshape(n, total, 512), *earlier.values())
    return dict(zip(used, new))


CORES = 2
PARTS = 4


def part_rows(total):
    long = -(-total // (2 * 16 * 2)) * 16
    short = total // 2 - long
    return (0, long), (long, short), (total // 2, long), (total // 2 + long, short)


def reduce_kernel(g, out, mine, pair, sent, got, mine_sem, pair_send, pair_got, send_sem, got_sem):
    n, total = g.shape[0], g.shape[1]
    chips = n // CORES
    far, parts = chips // 2, part_rows(total)
    me = lax.axis_index("dp")
    z, core = lax.div(me, CORES), lax.rem(me, CORES)
    at = lambda chip, which: {"dp": lax.rem(chip + chips, chips) * CORES + which}
    peers = {1: at(z + 1, core), -1: at(z - 1, core)}
    partner = at(z, 1 - core)

    barrier = pltpu.get_barrier_semaphore()
    for peer in (peers[1], peers[-1], partner):
        pl.semaphore_signal(barrier, inc=1, device_id=peer, device_id_type=pl.DeviceIdType.MESH)

    order = [far] + [x * sign for x in range(far - 1, 0, -1) for sign in (1, -1)] + [0]
    slot = {offset: i for i, offset in enumerate(order)} | {-far: 0}
    local = []
    for i, offset in enumerate(order):
        chunk = lax.rem(z + offset + chips, chips) * CORES
        local.append(pltpu.make_async_copy(g.at[chunk + core], mine.at[i], mine_sem.at[i]))
        local[i].start()
    pl.semaphore_wait(barrier, 3)
    across = []
    for i, offset in enumerate(order):
        chunk = lax.rem(z + offset + chips, chips) * CORES
        across.append(pltpu.make_async_remote_copy(g.at[chunk + 1 - core], pair.at[i], pair_send.at[i], pair_got.at[i], device_id=partner,
                                                   device_id_type=pl.DeviceIdType.MESH))
        across[i].start()

    streams = [(sign, part, far if (part < PARTS // 2) == (sign > 0) else far - 1) for part in range(PARTS) for sign in (1, -1)]
    ready, copies = set(), {}

    def own(offset, here):
        i = slot[offset]
        if i not in ready:
            ready.add(i)
            local[i].wait()
            across[i].wait_recv()
        return mine[i, here, :].astype(F32) + pair[i, here, :].astype(F32)

    for s in range(far):
        pending = None
        for x, (sign, part, hops) in enumerate(streams):
            if s < hops:
                value = own(sign * (hops - s), pl.ds(*parts[part]))
                if s:
                    copies[s - 1, x].wait_recv()
                    value = value + got[s - 1, x, : parts[part][1]].astype(F32)
                many = pl.ds(0, parts[part][1])
                sent[s, x, many] = value.astype(LOW)
                copies[s, x] = pltpu.make_async_remote_copy(sent.at[s, x, many], got.at[s, x, many], send_sem.at[s, x], got_sem.at[s, x],
                                                            device_id=peers[sign], device_id_type=pl.DeviceIdType.MESH)
                if pending is not None:
                    pending.start()
                pending = copies[s, x]
        pending.start()
    for part in range(PARTS):
        here = pl.ds(*parts[part])
        value = own(0, here)
        for x, (_, of, hops) in enumerate(streams):
            if of == part:
                copies[hops - 1, x].wait_recv()
                value = value + got[hops - 1, x, : parts[part][1]].astype(F32)
        out[here, :] = value.astype(LOW)
    for copy in (*across, *copies.values()):
        copy.wait_send()


def reduce(g):
    n, total, width = g.shape
    chips = n // CORES
    far, streams = chips // 2, 2 * PARTS
    out = jax.ShapeDtypeStruct((total, width), LOW)
    dma = lambda *shape: pltpu.SemaphoreType.DMA(shape)
    return pl.pallas_call(
        reduce_kernel,
        in_specs=[pl.BlockSpec(memory_space=pl.ANY)],
        out_specs=pl.BlockSpec(memory_space=pltpu.VMEM),
        out_shape=out,
        scratch_shapes=[pltpu.VMEM((chips, total, width), LOW)] * 2 + [pltpu.VMEM((far, streams, part_rows(total)[0][1], width), LOW)] * 2
        + [dma(chips)] * 3 + [dma(far, streams)] * 2,
        compiler_params=pltpu.CompilerParams(collective_id=1, has_side_effects=True, vmem_limit_bytes=VMEM),
        cost_estimate=pl.CostEstimate(flops=50_000_000_000, transcendentals=0, bytes_accessed=g.size * 2),
        name="reduce",
    )(g)


def solution(mesh):
    n = mesh.shape["dp"]

    def scatter(g):
        return lax.psum_scatter(g.reshape(-1, g.shape[2]), "dp", scatter_dimension=0, tiled=True)

    def step(x, dy, *arrays):
        weights, m, v = (arrays[i : i + 7] for i in (0, 7, 14))
        wq, wk, wv, wo, wg, wu, wd = weights
        h0, t = x[0], x.shape[1]
        half = HEAD // 2
        rate = THETA ** (-jnp.arange(half, dtype=F32) / half)
        high = (jnp.arange(t // 64, dtype=F32) * 64)[:, None, None] * rate
        low = jnp.arange(64, dtype=F32)[:, None] * rate
        ch, sh, cl, sl = lax.optimization_barrier((jnp.cos(high), jnp.sin(high), jnp.cos(low), jnp.sin(low)))
        cos, sin = (ch * cl - sh * sl).reshape(t, half), (sh * cl + ch * sl).reshape(t, half)
        me = lax.axis_index("dp").astype(jnp.int32).reshape(1)
        q0, k0, v0 = first(h0, wq, wk, wv, cos, sin, 0)
        c0, l0 = attention(q0, k0, v0)
        h1, q1, k1, v1 = middle(c0, h0, wo, wg, wu, wd, wq, wk, wv, cos, sin, 0)
        c1, l1 = attention(q1, k1, v1)
        by, by_c, g1 = mlp_back(c1, h1, dy[0], wo, wg, wu, wd, 1, n)
        r1 = scatter(g1)
        by, late = attention_back(q1, k1, v1, by_c, c1, l1, h1, cos, sin, n, 1, by, wq, wk, wv)
        by, by_c, g0 = mlp_back(c0, h0, by, wo, wg, wu, wd, 0, n, 2 * late.shape[1])
        new1, moments = adamw(me, r1, weights, m, v, LATE, after=(by_c,))
        all1 = lax.all_gather(new1, "dp", axis=0, tiled=True)
        (g0,) = attention_back(q0, k0, v0, by_c, c0, l0, h0, cos, sin, n, 0, packed=g0, late=late, after=(new1,))
        new0, moments = adamw(me, reduce(g0), weights, m, v, EARLY, moments)
        all0 = lax.all_gather(new0, "dp", axis=0, tiled=True)
        new = unpack(all0, weights, n, EARLY, unpack(all1, weights, n, LATE))
        return tuple(new[i] for i in range(7)) + tuple(moments[i][which] for which in range(2) for i in range(7))

    states, all_of, cut = P(("rep", "dp"), None, None), P(None, None, None), P(None, "dp", None)
    return jax.shard_map(
        step,
        mesh=mesh,
        in_specs=(states, states) + (all_of,) * 7 + (cut,) * 14,
        out_specs=(P("rep", None, None),) * 7 + (P("rep", "dp", None),) * 14,
        check_vma=False,
    )
```

```python
import functools

import jax
import jax.numpy as jnp
from jax import lax
from jax.experimental import pallas as pl
from jax.experimental.pallas import tpu as pltpu
from jax.sharding import PartitionSpec as P

HEAD = 256
THETA = 10000
EPS = 1e-6
HIDDEN = -2e30
LOG2E = 1.4426950408889634
LN2 = 0.6931471805599453
STRIP = 512
ROWS = 512
LOW = jnp.bfloat16
F32 = jnp.float32
LATE = tuple((i, 1) for i in (3, 4, 5, 6))
EARLY = tuple((i, 0) for i in (3, 4, 5, 6, 0, 1, 2)) + tuple((i, 1) for i in (0, 1, 2))


def dot(a, b, ca=1, cb=0):
    return lax.dot_general(a, b, (((ca,), (cb,)), ((), ())), preferred_element_type=F32)


def params(mib):
    return pltpu.CompilerParams(dimension_semantics=("arbitrary",), vmem_limit_bytes=mib * 2**20)


def cost(flops, *arrays):
    return pl.CostEstimate(flops=int(flops), transcendentals=0, bytes_accessed=sum(a.size * a.dtype.itemsize for a in arrays))


def spread(h):
    wide = h.astype(F32)
    return wide, lax.rsqrt(jnp.mean(wide * wide, -1, keepdims=True) + EPS)


def norm_back(wide, scale, by):
    return scale * by - wide * (scale * scale * scale * jnp.mean(by * wide, -1, keepdims=True))


def turn(t, cos, sin):
    half, out = HEAD // 2, []
    for at in range(0, t.shape[1], HEAD):
        a, b = t[:, at : at + half].astype(F32), t[:, at + half : at + HEAD].astype(F32)
        out += [a * cos - b * sin, b * cos + a * sin]
    return jnp.concatenate(out, -1).astype(LOW)


def queries_keys_values(h, wq, wk, wv, cos, sin, q_ref, k_ref, v_ref):
    wide, scale = spread(h)
    a = (wide * scale).astype(LOW)
    q_ref[...] = turn(dot(a, wq[0]).astype(LOW), cos[...], sin[...])
    k_ref[...] = turn(dot(a, wk[0]).astype(LOW), cos[...], sin[...])
    v_ref[...] = dot(a, wv[0]).astype(LOW)


def matrix(w, layer):
    return pl.BlockSpec((1,) + w.shape[1:], lambda *_: (layer, 0, 0), pipeline_mode=pl.Buffered(1))


def rows(width, at=ROWS):
    return pl.BlockSpec((at, width), lambda i: (i, 0))


def first_kernel(h, wq, wk, wv, cos, sin, q_ref, k_ref, v_ref):
    queries_keys_values(h[...], wq, wk, wv, cos, sin, q_ref, k_ref, v_ref)


def first(h, wq, wk, wv, cos, sin, layer):
    t, d = h.shape
    n = wq.shape[2]
    outs = [jax.ShapeDtypeStruct((t, n), LOW)] * 3
    return pl.pallas_call(
        first_kernel,
        grid=(t // ROWS,),
        in_specs=[rows(d), matrix(wq, layer), matrix(wk, layer), matrix(wv, layer), rows(HEAD // 2), rows(HEAD // 2)],
        out_specs=[rows(n)] * 3,
        out_shape=outs,
        compiler_params=params(12),
        cost_estimate=cost(6 * t * d * n, h, *outs),
        name="qkv",
    )(h, wq, wk, wv, cos, sin)


def mlp_chunk(b, wg, wu, at, size):
    gate = dot(b, wg[0, :, at : at + size])
    up = dot(b, wu[0, :, at : at + size])
    return gate, up, 0.5 * jnp.tanh(0.5 * gate) + 0.5


def middle_kernel(ctx, h, wo, wg, wu, wd, wq, wk, wv, cos, sin, out_ref, q_ref, k_ref, v_ref):
    h1 = (h[...].astype(F32) + dot(ctx[...], wo[0]).astype(LOW).astype(F32)).astype(LOW)
    wide, scale = spread(h1)
    b = (wide * scale).astype(LOW)
    ff, size = wg.shape[2], 512
    acts = []
    for at in range(0, ff, size):
        gate, up, s = mlp_chunk(b, wg, wu, at, size)
        acts.append((gate * s * up).astype(LOW))
    down = dot(jnp.concatenate(acts, -1), wd[0])
    h2 = (wide + down.astype(LOW).astype(F32)).astype(LOW)
    out_ref[...] = h2
    queries_keys_values(h2, wq, wk, wv, cos, sin, q_ref, k_ref, v_ref)


def middle(ctx, h, wo, wg, wu, wd, wq, wk, wv, cos, sin, layer):
    t, d = h.shape
    n, ff = wq.shape[2], wg.shape[2]
    outs = [jax.ShapeDtypeStruct((t, d), LOW)] + [jax.ShapeDtypeStruct((t, n), LOW)] * 3
    return pl.pallas_call(
        middle_kernel,
        grid=(t // ROWS,),
        in_specs=[rows(n), rows(d)] + [matrix(w, layer) for w in (wo, wg, wu, wd)] + [matrix(w, layer + 1) for w in (wq, wk, wv)]
        + [rows(HEAD // 2)] * 2,
        out_specs=[rows(d)] + [rows(n)] * 3,
        out_shape=outs,
        compiler_params=params(30),
        cost_estimate=cost(2 * t * d * (4 * n + 3 * ff), h, h, *outs),
        name="middle",
    )(ctx, h, wo, wg, wu, wd, wq, wk, wv, cos, sin)


def causal_mask(size):
    return lax.broadcasted_iota(jnp.int32, (size, size), 1) >= lax.broadcasted_iota(jnp.int32, (size, size), 0)


def attention_kernel(q_ref, k_ref, v_ref, o_ref, lse_ref, mix_s, top_s):
    t, d = q_ref.shape
    e = d**-0.5 * LOG2E
    ones = jnp.ones((8, STRIP), LOW)
    blocks = [pl.ds(at, STRIP) for at in range(0, t, STRIP)]
    for j, keys in enumerate(blocks):
        k = k_ref[keys, :]
        values = jnp.concatenate([v_ref[keys, :].T, ones], axis=0)
        seen = blocks[j:]
        scores = [dot(k, q_ref[qs, :], 1, 1) for qs in seen]
        weights, keeps = [], []
        for qs, s in zip(seen, scores):
            if qs is keys:
                s = jnp.where(causal_mask(STRIP), s, HIDDEN)
            top = s.max(axis=0, keepdims=True)
            if j:
                old = top_s[0:1, qs]
                top = jnp.maximum(old, top)
                keeps.append(jnp.exp2((old - top) * e))
            top_s[0:1, qs] = top
            weights.append(jnp.exp2((s - top) * e).astype(LOW))
        for n, (qs, p) in enumerate(zip(seen, weights)):
            new = dot(values, p, 1, 0)
            if j:
                new = mix_s[:, qs] * keeps[n] + new
            if qs is keys:
                total = new[d : d + 1, :]
                o_ref[qs, :] = (new[:d, :] * (1 / total)).T.astype(LOW)
                lse_ref[0, :, qs] = top_s[0:1, qs] * e + jnp.log(total) * LOG2E
            else:
                mix_s[:, qs] = new


def head_specs(t, count):
    return [pl.BlockSpec((t, HEAD), lambda i: (0, i))] * count


def attention(q, k, v):
    t, n = q.shape
    outs = [jax.ShapeDtypeStruct((t, n), LOW), jax.ShapeDtypeStruct((n // HEAD, 1, t), F32)]
    return pl.pallas_call(
        attention_kernel,
        grid=(n // HEAD,),
        in_specs=head_specs(t, 3),
        out_specs=[*head_specs(t, 1), pl.BlockSpec((1, 1, t), lambda i: (i, 0, 0))],
        out_shape=outs,
        scratch_shapes=[pltpu.VMEM((HEAD + 8, t), F32), pltpu.VMEM((8, t), F32)],
        compiler_params=params(24),
        cost_estimate=cost(2.5 * t * t * n, q, k, v, *outs),
        name="attention",
    )(q, k, v)


def attention_back_kernel(q_ref, k_ref, v_ref, do_ref, o_ref, lse_ref, h, cos, sin, *rest, deeper):
    if deeper:
        by_h1_in, wq, wk, wv = rest[:4]
        by_h, grads, dq_s, at_s, by_q, by_k, by_v, mine, sem, h_s, cos_s, sin_s, by_h1, by_a = rest[4:]
    else:
        late = rest[1]
        grads, dq_s, at_s, by_q, by_k, by_v, mine, sem, h_s, cos_s, sin_s = rest[-11:]
    fetches = [pltpu.make_async_copy(x, to, sem.at[2 + i]) for i, (x, to) in enumerate(((cos, cos_s), (sin, sin_s), (h, h_s)))]
    if deeper:
        fetches.append(pltpu.make_async_copy(by_h1_in, by_h1, sem.at[5]))
    h, cos, sin = h_s, cos_s, sin_s
    t, d = q_ref.shape
    n, head = grads.shape[0], pl.program_id(0)
    scale = d**-0.5
    e = scale * LOG2E
    blocks = [pl.ds(at, STRIP) for at in range(0, t, STRIP)]

    @pl.when(head == 0)
    def _():
        for fetch in fetches:
            fetch.start()

    deltas = []
    for qs in blocks:
        both = do_ref[qs, :].astype(F32) * o_ref[qs, :].astype(F32)
        folded = sum(both[:, at : at + 128] for at in range(0, d, 128))
        deltas.append(folded.T.sum(axis=0, keepdims=True))

    @pl.when(head == 0)
    def _():
        for fetch in fetches[:2]:
            fetch.wait()

    for j, keys in enumerate(blocks):
        k, v = k_ref[keys, :], v_ref[keys, :]
        kt = k.T
        seen = list(enumerate(blocks))[j:]
        scores = [dot(k, q_ref[qs, :], 1, 1) for _, qs in seen]
        dps = [dot(v, do_ref[qs, :], 1, 1) for _, qs in seen]
        ps, dss = [], []
        for m, (x, qs) in enumerate(seen):
            p = jnp.exp2(scores[m] * e - lse_ref[0, :, qs])
            if x == j:
                p = jnp.where(causal_mask(STRIP), p, 0.0)
            ds = (p * (dps[m] - deltas[x])).astype(LOW)
            ps.append(p.astype(LOW))
            dss.append(ds)
            new = dot(kt, ds, 1, 0)
            if j:
                new = dq_s[:, qs] + new
            if x == j:
                by_q[qs, :] = turn((new * scale).T.astype(LOW), cos[qs, :], -sin[qs, :])
            else:
                dq_s[:, qs] = new
        late_q = pl.ds(j * STRIP, t - j * STRIP)
        by_v[keys, :] = dot(jnp.concatenate(ps, axis=1), do_ref[late_q, :], 1, 0).astype(LOW)
        dk = (dot(jnp.concatenate(dss, axis=1), q_ref[late_q, :], 1, 0) * scale).astype(LOW)
        by_k[keys, :] = turn(dk, cos[keys, :], -sin[keys, :])

    @pl.when(head == 0)
    def _():
        for fetch in fetches[2:]:
            fetch.wait()
        for qs in blocks:
            wide, size = spread(h[qs, :])
            at_s[:, qs] = (wide * size).astype(LOW).T

    r = at_s.shape[0] // n
    for i, by in enumerate((by_q, by_k, by_v)):
        mine[:, i * r : (i + 1) * r, :] = dot(at_s[...], by[...]).reshape(n, r, d).astype(LOW)
    base = 0 if deeper else grads.shape[1] - 6 * r
    copies = [pltpu.make_async_copy(mine, grads.at[:, pl.ds(base, 3 * r), pl.ds(pl.multiple_of(head * d, d), d)], sem.at[0])]
    copies[0].start()
    if not deeper:
        copies.append(pltpu.make_async_copy(late, grads.at[:, pl.ds(base + 3 * r, 3 * r), :], sem.at[1]))

        @pl.when(head == 0)
        def _():
            copies[1].start()
            copies[1].wait()
    else:
        for qs in blocks:
            term = dot(by_q[qs, :], wq[0], 1, 1) + dot(by_k[qs, :], wk[0], 1, 1) + dot(by_v[qs, :], wv[0], 1, 1)
            by_a[qs, :] = jnp.where(head == 0, term, by_a[qs, :] + term)

        @pl.when(head == pl.num_programs(0) - 1)
        def _():
            for qs in blocks:
                wide, size = spread(h[qs, :])
                back = norm_back(wide, size, by_a[qs, :].astype(LOW).astype(F32)).astype(LOW).astype(F32)
                by_h[qs, :] = (by_h1[qs, :].astype(F32) + back).astype(LOW)
    copies[0].wait()


def attention_back(q, k, v, by, out, lse, h, cos, sin, n, layer, by_h1=None, wq=None, wk=None, wv=None, packed=None, late=None, after=()):
    t, width = q.shape
    d = h.shape[1]
    deeper = packed is None
    once = lambda a: pl.BlockSpec(a.shape, lambda i: (0,) * a.ndim, pipeline_mode=pl.Buffered(1))
    anywhere = pl.BlockSpec(memory_space=pl.ANY)
    given = [q, k, v, by, out, lse, h, cos, sin]
    specs = [*head_specs(t, 5), pl.BlockSpec((1, 1, t), lambda i: (i, 0, 0))] + [anywhere] * 3
    scratch = [pltpu.VMEM((HEAD, t), F32), pltpu.VMEM((d, t), LOW)] + [pltpu.VMEM((t, HEAD), LOW)] * 3
    scratch += [pltpu.VMEM((n, 3 * d // n, HEAD), LOW), pltpu.SemaphoreType.DMA((6,))]
    scratch += [pltpu.VMEM((t, d), LOW)] + [pltpu.VMEM(cos.shape, F32)] * 2
    if deeper:
        given += [by_h1, wq, wk, wv]
        specs += [anywhere] + [pl.BlockSpec((1, d, HEAD), lambda i: (layer, 0, i))] * 3
        outs = [jax.ShapeDtypeStruct((t, d), LOW), jax.ShapeDtypeStruct((n, 3 * d // n, width), LOW)]
        out_specs = [once(h), anywhere]
        scratch += [pltpu.VMEM((t, d), LOW), pltpu.VMEM((t, d), F32)]
    else:
        given += [packed, late, *after]
        specs += [anywhere, once(late)] + [anywhere] * len(after)
        outs, out_specs = [jax.ShapeDtypeStruct(packed.shape, LOW)], [anywhere]
    return pl.pallas_call(
        functools.partial(attention_back_kernel, deeper=deeper),
        grid=(width // HEAD,),
        in_specs=specs,
        out_specs=out_specs,
        out_shape=outs,
        scratch_shapes=scratch,
        input_output_aliases={} if deeper else {9: 0},
        compiler_params=params(62),
        cost_estimate=cost(6.25 * t * t * width + 2 * t * d * width * (6 if deeper else 3), q, k, v, by, out, h, h),
        name="attention_back",
    )(*given)


def mlp_back_kernel(ctx, h, by, wo, wg_in, wu_in, wd_in, by_h1, by_ctx, grads, acc_o, acc_g, acc_u, acc_d, b_s, bt_s, dyt_s, by_b, stage, sems,
                    wg, wu, wd, fetched, *, layer):
    step = pl.program_id(0)

    def fetches(c):
        here = pl.ds(pl.multiple_of(c * CHUNK, CHUNK), CHUNK)
        return [pltpu.make_async_copy(wg_in.at[layer, :, here], wg.at[0, :, here], fetched.at[0, c]),
                pltpu.make_async_copy(wu_in.at[layer, :, here], wu.at[0, :, here], fetched.at[1, c]),
                pltpu.make_async_copy(wd_in.at[layer, here, :], wd.at[0, here, :], fetched.at[2, c])]

    @pl.when(step == 0)
    def _():
        for c in range(wg.shape[2] // CHUNK):
            for fetch in fetches(c):
                fetch.start()

    last = step == pl.num_programs(0) - 1
    n, d, ff = grads.shape[0], wg.shape[1], wg.shape[2]
    r, rd, chunks = d // n, ff // n, ff // CHUNK
    many = CHUNK // rd

    def put(acc, where, term):
        acc[where] = jnp.where(step == 0, term, acc[where] + term)

    def leave(owners, first, count, i, kind):
        where = (owners, pl.ds(first, count))
        return pltpu.make_async_copy(stage.at[where], grads.at[where], sems.at[kind, i])

    def leaving(c):
        gate_rows = pl.multiple_of(r + c * r, r)
        up_rows = pl.multiple_of(r + (chunks + c) * r, r)
        owners = pl.ds(pl.multiple_of(c * many, many), many)
        return gate_rows, up_rows, owners, (leave(pl.ds(0, n), gate_rows, r, c, 0), leave(pl.ds(0, n), up_rows, r, c, 1),
                                            leave(owners, r * (1 + 2 * chunks), rd, c, 2))

    h1 = (h[...].astype(F32) + dot(ctx[...], wo[0]).astype(LOW).astype(F32)).astype(LOW)
    wide, scale = spread(h1)
    b = (wide * scale).astype(LOW)
    b_s[...] = b
    bt_s[...] = b.T
    dyt_s[...] = by[...].T
    by_b[...] = jnp.zeros(by_b.shape, F32)

    def chunk(c):
        here = pl.ds(pl.multiple_of(c * CHUNK, CHUNK), CHUNK)
        gate, up = dot(b_s[...], wg[0, :, here]), dot(b_s[...], wu[0, :, here])
        s = 0.5 * jnp.tanh(0.5 * gate) + 0.5
        by_act = dot(by[...], wd[0, here, :], 1, 1).astype(LOW).astype(F32)
        silu = gate * s
        act = (silu * up).astype(LOW)
        by_up = (by_act * silu).astype(LOW)
        by_gate = (by_act * up * (s + silu * (1.0 - s))).astype(LOW)
        by_b[...] += dot(by_gate, wg[0, :, here], 1, 1) + dot(by_up, wu[0, :, here], 1, 1)
        put(acc_d, (slice(None), here), dot(dyt_s[...], act))
        put(acc_g, (slice(None), here), dot(bt_s[...], by_gate))
        put(acc_u, (slice(None), here), dot(bt_s[...], by_up))

    def two(i, _):
        @pl.when(step == 0)
        def _():
            for c in (2 * i, 2 * i + 1):
                for fetch in fetches(c):
                    fetch.wait()

        for c in (2 * i, 2 * i + 1):
            chunk(c)

        @pl.when(last)
        def _():
            for c in (2 * i, 2 * i + 1):
                here = pl.ds(pl.multiple_of(c * CHUNK, CHUNK), CHUNK)
                gate_rows, up_rows, owners, copies = leaving(c)
                stage[:, pl.ds(gate_rows, r), :] = acc_g[:, here].reshape(n, r, CHUNK).astype(LOW)
                stage[:, pl.ds(up_rows, r), :] = acc_u[:, here].reshape(n, r, CHUNK).astype(LOW)
                stage[owners, r * (1 + 2 * chunks) :, :] = acc_d[:, here].T.reshape(many, rd, d).astype(LOW)
                for copy in copies:
                    copy.start()

    lax.fori_loop(0, chunks // 2, two, None)
    wide, scale = spread(h1)
    total = (by[...].astype(F32) + norm_back(wide, scale, by_b[...].astype(LOW).astype(F32)).astype(LOW).astype(F32)).astype(LOW)
    by_h1[...] = total
    by_ctx[...] = dot(total, wo[0], 1, 1).astype(LOW)
    put(acc_o, (slice(None), slice(None)), dot(ctx[...].T, total))

    @pl.when(last)
    def _():
        stage[:, :r, :] = acc_o[...].reshape(n, r, d).astype(LOW)
        copy = leave(pl.ds(0, n), 0, r, 0, 3)
        copy.start()
        for c in range(chunks):
            for each in leaving(c)[3]:
                each.wait()
        copy.wait()


CHUNK = 512


def mlp_back(ctx, h, by, wo, wg, wu, wd, layer, n, room=0, size=512):
    t, d = h.shape
    heads, ff = wo.shape[1], wg.shape[2]
    packed = (heads * d + 3 * d * ff) // (512 * n)
    outs = [jax.ShapeDtypeStruct((t, d), LOW), jax.ShapeDtypeStruct((t, heads), LOW), jax.ShapeDtypeStruct((n, packed + room, 512), LOW)]
    return pl.pallas_call(
        functools.partial(mlp_back_kernel, layer=layer),
        grid=(t // size,),
        in_specs=[rows(heads, size), rows(d, size), rows(d, size), matrix(wo, layer)] + [pl.BlockSpec(memory_space=pl.ANY)] * 3,
        out_specs=[rows(d, size), rows(heads, size), pl.BlockSpec(memory_space=pl.ANY)],
        out_shape=outs,
        scratch_shapes=[pltpu.VMEM((heads, d), F32)] + [pltpu.VMEM((d, ff), F32)] * 3
        + [pltpu.VMEM((size, d), LOW), pltpu.VMEM((d, size), LOW), pltpu.VMEM((d, size), LOW), pltpu.VMEM((size, d), F32)]
        + [pltpu.VMEM((n, packed, 512), LOW), pltpu.SemaphoreType.DMA((4, ff // CHUNK))]
        + [pltpu.VMEM((1,) + w.shape[1:], LOW) for w in (wg, wu, wd)] + [pltpu.SemaphoreType.DMA((3, ff // CHUNK))],
        compiler_params=params(62),
        cost_estimate=cost(2 * t * d * (8 * ff + 3 * heads), h, h, h, *outs),
        name="mlp_back",
    )(ctx, h, by, wo, wg, wu, wd)


def layers_of(plan):
    return {i: [layer for j, layer in plan if j == i] for i in sorted({i for i, _ in plan})}


def adamw_kernel(me, packed_g, *refs, plan):
    used = layers_of(plan)
    count = len(used)
    ws, ms, vs = (dict(zip(used, refs[k * count : (k + 1) * count])) for k in range(3))
    rest = refs[-1 - 2 * count :]
    packed, new_m, new_v = rest[0], dict(zip(used, rest[1 : 1 + count])), dict(zip(used, rest[1 + count :]))
    at = 0
    for i, layer in plan:
        x = layer - used[i][0]
        r, width = ms[i].shape[1], ms[i].shape[2]
        for c in range(0, width, 512):
            cols = slice(c, c + 512)
            g = packed_g[at : at + r, :].astype(F32)
            m = 0.9 * ms[i][x, :, cols] + 0.1 * g
            v = 0.95 * vs[i][x, :, cols] + 0.05 * g * g
            w = ws[i][x, :, cols].astype(F32)
            new_m[i][x, :, cols] = m
            new_v[i][x, :, cols] = v
            packed[at : at + r, :] = (w - 0.02 * (m * lax.rsqrt(v + 1e-8) + 0.1 * w)).astype(LOW)
            at += r


def adamw(me, g, ws, ms, vs, plan, earlier=None, after=()):
    used, earlier = layers_of(plan), earlier or {}
    spec = lambda i, mine: pl.BlockSpec((len(used[i]),) + ms[i].shape[1:], lambda _, me: (used[i][0], me[0] if mine else 0, 0))
    own, part = [spec(i, True) for i in used], [spec(i, False) for i in used]
    total = g.shape[0]
    outs = [jax.ShapeDtypeStruct((total, 512), LOW)] + [jax.ShapeDtypeStruct(ms[i].shape, F32) for _ in range(2) for i in used]
    known = [earlier[i][k] for k in range(2) for i in earlier]
    given = [g] + [a[i] for a in (ws, ms, vs) for i in used] + known + list(after)
    first = 2 + 3 * len(used)
    to = [1 + k * len(used) + list(used).index(i) for k in range(2) for i in earlier]
    new, *moments = pl.pallas_call(
        functools.partial(adamw_kernel, plan=plan),
        grid_spec=pltpu.PrefetchScalarGridSpec(
            num_scalar_prefetch=1,
            grid=(1,),
            in_specs=[pl.BlockSpec(g.shape, lambda _, me: (0, 0)), *own, *part, *part] + [pl.BlockSpec(memory_space=pl.ANY)] * len([*known, *after]),
            out_specs=[pl.BlockSpec((total, 512), lambda _, me: (0, 0)), *part, *part],
        ),
        out_shape=outs,
        input_output_aliases={first + i: o for i, o in enumerate(to)},
        compiler_params=params(54 if earlier else 62),
        cost_estimate=cost(20 * total * 512, g, *outs),
        name="adamw",
    )(me, *given)
    return new, {i: (moments[x], moments[x + len(used)]) for x, i in enumerate(used)}


def unpack_kernel(packed, *refs, plan):
    used = layers_of(plan)
    outs, at = dict(zip(used, refs[-len(used) :])), 0
    owners = packed.shape[0]
    for i, layer in plan:
        out = outs[i]
        r = out.shape[1] // owners
        for c in range(0, out.shape[2], 512):
            for owner in range(owners):
                out[layer - used[i][0], owner * r : (owner + 1) * r, c : c + 512] = packed[owner, at : at + r, :]
            at += r


def unpack(packed, ws, n, plan, earlier=None):
    used, earlier = layers_of(plan), earlier or {}
    outs = [jax.ShapeDtypeStruct(ws[i].shape, LOW) for i in used]
    total = packed.shape[0] // n
    some = min(n, 4)
    new = pl.pallas_call(
        functools.partial(unpack_kernel, plan=plan),
        grid=(n // some,),
        in_specs=[pl.BlockSpec((some, total, 512), lambda i: (i, 0, 0))] + [pl.BlockSpec(memory_space=pl.ANY)] * len(earlier),
        out_specs=[pl.BlockSpec((len(used[i]), some * ws[i].shape[1] // n, ws[i].shape[2]), lambda at, i=i: (used[i][0], at, 0)) for i in used],
        out_shape=outs,
        input_output_aliases={1 + x: list(used).index(i) for x, i in enumerate(earlier)},
        compiler_params=params(62),
        cost_estimate=cost(0, *outs),
        name="unpack",
    )(packed.reshape(n, total, 512), *earlier.values())
    return dict(zip(used, new))


CORES = 2
PARTS = 4


def part_rows(total):
    long = -(-total // (2 * 16 * 2)) * 16
    short = total // 2 - long
    return (0, long), (long, short), (total // 2, long), (total // 2 + long, short)


def reduce_kernel(g, out, mine, pair, sent, got, mine_sem, pair_send, pair_got, send_sem, got_sem):
    n, total = g.shape[0], g.shape[1]
    chips = n // CORES
    far, parts = chips // 2, part_rows(total)
    me = lax.axis_index("dp")
    z, core = lax.div(me, CORES), lax.rem(me, CORES)
    at = lambda chip, which: {"dp": lax.rem(chip + chips, chips) * CORES + which}
    peers = {1: at(z + 1, core), -1: at(z - 1, core)}
    partner = at(z, 1 - core)

    barrier = pltpu.get_barrier_semaphore()
    for peer in (peers[1], peers[-1], partner):
        pl.semaphore_signal(barrier, inc=1, device_id=peer, device_id_type=pl.DeviceIdType.MESH)

    order = [far] + [x * sign for x in range(far - 1, 0, -1) for sign in (1, -1)] + [0]
    slot = {offset: i for i, offset in enumerate(order)} | {-far: 0}
    local = []
    for i, offset in enumerate(order):
        chunk = lax.rem(z + offset + chips, chips) * CORES
        local.append(pltpu.make_async_copy(g.at[chunk + core], mine.at[i], mine_sem.at[i]))
        local[i].start()
    pl.semaphore_wait(barrier, 3)
    across = []
    for i, offset in enumerate(order):
        chunk = lax.rem(z + offset + chips, chips) * CORES
        across.append(pltpu.make_async_remote_copy(g.at[chunk + 1 - core], pair.at[i], pair_send.at[i], pair_got.at[i], device_id=partner,
                                                   device_id_type=pl.DeviceIdType.MESH))
        across[i].start()

    streams = [(sign, part, far if (part < PARTS // 2) == (sign > 0) else far - 1) for part in range(PARTS) for sign in (1, -1)]
    ready, copies = set(), {}

    def own(offset, here):
        i = slot[offset]
        if i not in ready:
            ready.add(i)
            local[i].wait()
            across[i].wait_recv()
        return mine[i, here, :].astype(F32) + pair[i, here, :].astype(F32)

    for s in range(far):
        pending = None
        for x, (sign, part, hops) in enumerate(streams):
            if s < hops:
                value = own(sign * (hops - s), pl.ds(*parts[part]))
                if s:
                    copies[s - 1, x].wait_recv()
                    value = value + got[s - 1, x, : parts[part][1]].astype(F32)
                many = pl.ds(0, parts[part][1])
                sent[s, x, many] = value.astype(LOW)
                copies[s, x] = pltpu.make_async_remote_copy(sent.at[s, x, many], got.at[s, x, many], send_sem.at[s, x], got_sem.at[s, x],
                                                            device_id=peers[sign], device_id_type=pl.DeviceIdType.MESH)
                if pending is not None:
                    pending.start()
                pending = copies[s, x]
        pending.start()
    for part in range(PARTS):
        here = pl.ds(*parts[part])
        value = own(0, here)
        for x, (_, of, hops) in enumerate(streams):
            if of == part:
                copies[hops - 1, x].wait_recv()
                value = value + got[hops - 1, x, : parts[part][1]].astype(F32)
        out[here, :] = value.astype(LOW)
    for copy in (*across, *copies.values()):
        copy.wait_send()


def reduce(g):
    n, total, width = g.shape
    chips = n // CORES
    far, streams = chips // 2, 2 * PARTS
    out = jax.ShapeDtypeStruct((total, width), LOW)
    dma = lambda *shape: pltpu.SemaphoreType.DMA(shape)
    return pl.pallas_call(
        reduce_kernel,
        in_specs=[pl.BlockSpec(memory_space=pl.ANY)],
        out_specs=pl.BlockSpec(memory_space=pltpu.VMEM),
        out_shape=out,
        scratch_shapes=[pltpu.VMEM((chips, total, width), LOW)] * 2 + [pltpu.VMEM((far, streams, part_rows(total)[0][1], width), LOW)] * 2
        + [dma(chips)] * 3 + [dma(far, streams)] * 2,
        compiler_params=pltpu.CompilerParams(collective_id=1, has_side_effects=True, vmem_limit_bytes=55 * 2**20),
        cost_estimate=pl.CostEstimate(flops=50_000_000_000, transcendentals=0, bytes_accessed=g.size * 2),
        name="reduce",
    )(g)


def solution(mesh):
    n = mesh.shape["dp"]

    def scatter(g):
        return lax.psum_scatter(g.reshape(-1, g.shape[2]), "dp", scatter_dimension=0, tiled=True)

    def step(x, dy, *arrays):
        weights, m, v = (arrays[i : i + 7] for i in (0, 7, 14))
        wq, wk, wv, wo, wg, wu, wd = weights
        h0, t = x[0], x.shape[1]
        half = HEAD // 2
        rate = THETA ** (-jnp.arange(half, dtype=F32) / half)
        high = (jnp.arange(t // 64, dtype=F32) * 64)[:, None, None] * rate
        low = jnp.arange(64, dtype=F32)[:, None] * rate
        ch, sh, cl, sl = lax.optimization_barrier((jnp.cos(high), jnp.sin(high), jnp.cos(low), jnp.sin(low)))
        cos, sin = (ch * cl - sh * sl).reshape(t, half), (sh * cl + ch * sl).reshape(t, half)
        me = lax.axis_index("dp").astype(jnp.int32).reshape(1)
        q0, k0, v0 = first(h0, wq, wk, wv, cos, sin, 0)
        c0, l0 = attention(q0, k0, v0)
        h1, q1, k1, v1 = middle(c0, h0, wo, wg, wu, wd, wq, wk, wv, cos, sin, 0)
        c1, l1 = attention(q1, k1, v1)
        by, by_c, g1 = mlp_back(c1, h1, dy[0], wo, wg, wu, wd, 1, n)
        r1 = scatter(g1)
        by, late = attention_back(q1, k1, v1, by_c, c1, l1, h1, cos, sin, n, 1, by, wq, wk, wv)
        by, by_c, g0 = mlp_back(c0, h0, by, wo, wg, wu, wd, 0, n, 2 * late.shape[1])
        new1, moments = adamw(me, r1, weights, m, v, LATE, after=(by_c,))
        all1 = lax.all_gather(new1, "dp", axis=0, tiled=True)
        (g0,) = attention_back(q0, k0, v0, by_c, c0, l0, h0, cos, sin, n, 0, packed=g0, late=late, after=(new1,))
        new0, moments = adamw(me, reduce(g0), weights, m, v, EARLY, moments)
        all0 = lax.all_gather(new0, "dp", axis=0, tiled=True)
        new = unpack(all0, weights, n, EARLY, unpack(all1, weights, n, LATE))
        return tuple(new[i] for i in range(7)) + tuple(moments[i][which] for which in range(2) for i in range(7))

    states, all_of, cut = P(("rep", "dp"), None, None), P(None, None, None), P(None, "dp", None)
    return jax.shard_map(
        step,
        mesh=mesh,
        in_specs=(states, states) + (all_of,) * 7 + (cut,) * 14,
        out_specs=(P("rep", None, None),) * 7 + (P("rep", "dp", None),) * 14,
        check_vma=False,
    )
```

```python
import functools

import jax
import jax.numpy as jnp
from jax import lax
from jax.experimental import pallas as pl
from jax.experimental.pallas import tpu as pltpu
from jax.sharding import PartitionSpec as P

HEAD = 256
THETA = 10000
EPS = 1e-6
HIDDEN = -2e30
LOG2E = 1.4426950408889634
LN2 = 0.6931471805599453
STRIP = 512
ROWS = 512
LOW = jnp.bfloat16
F32 = jnp.float32
LATE = tuple((i, 1) for i in (3, 4, 5, 6))
EARLY = tuple((i, 0) for i in (3, 4, 5, 6, 0, 1, 2)) + tuple((i, 1) for i in (0, 1, 2))


def dot(a, b, ca=1, cb=0):
    return lax.dot_general(a, b, (((ca,), (cb,)), ((), ())), preferred_element_type=F32)


def params(mib):
    return pltpu.CompilerParams(dimension_semantics=("arbitrary",), vmem_limit_bytes=mib * 2**20)


def cost(flops, *arrays):
    return pl.CostEstimate(flops=int(flops), transcendentals=0, bytes_accessed=sum(a.size * a.dtype.itemsize for a in arrays))


def spread(h):
    wide = h.astype(F32)
    return wide, lax.rsqrt(jnp.mean(wide * wide, -1, keepdims=True) + EPS)


def norm_back(wide, scale, by):
    return scale * by - wide * (scale * scale * scale * jnp.mean(by * wide, -1, keepdims=True))


def turn(t, cos, sin):
    half, out = HEAD // 2, []
    for at in range(0, t.shape[1], HEAD):
        a, b = t[:, at : at + half].astype(F32), t[:, at + half : at + HEAD].astype(F32)
        out += [a * cos - b * sin, b * cos + a * sin]
    return jnp.concatenate(out, -1).astype(LOW)


def queries_keys_values(h, wq, wk, wv, cos, sin, q_ref, k_ref, v_ref):
    wide, scale = spread(h)
    a = (wide * scale).astype(LOW)
    q_ref[...] = turn(dot(a, wq[0]).astype(LOW), cos[...], sin[...])
    k_ref[...] = turn(dot(a, wk[0]).astype(LOW), cos[...], sin[...])
    v_ref[...] = dot(a, wv[0]).astype(LOW)


def matrix(w, layer):
    return pl.BlockSpec((1,) + w.shape[1:], lambda *_: (layer, 0, 0), pipeline_mode=pl.Buffered(1))


def rows(width, at=ROWS):
    return pl.BlockSpec((at, width), lambda i: (i, 0))


def first_kernel(h, wq, wk, wv, cos, sin, q_ref, k_ref, v_ref):
    queries_keys_values(h[...], wq, wk, wv, cos, sin, q_ref, k_ref, v_ref)


def first(h, wq, wk, wv, cos, sin, layer):
    t, d = h.shape
    n = wq.shape[2]
    outs = [jax.ShapeDtypeStruct((t, n), LOW)] * 3
    return pl.pallas_call(
        first_kernel,
        grid=(t // ROWS,),
        in_specs=[rows(d), matrix(wq, layer), matrix(wk, layer), matrix(wv, layer), rows(HEAD // 2), rows(HEAD // 2)],
        out_specs=[rows(n)] * 3,
        out_shape=outs,
        compiler_params=params(12),
        cost_estimate=cost(6 * t * d * n, h, *outs),
        name="qkv",
    )(h, wq, wk, wv, cos, sin)


def mlp_chunk(b, wg, wu, at, size):
    gate = dot(b, wg[0, :, at : at + size])
    up = dot(b, wu[0, :, at : at + size])
    return gate, up, 0.5 * jnp.tanh(0.5 * gate) + 0.5


def middle_kernel(ctx, h, wo, wg, wu, wd, wq, wk, wv, cos, sin, out_ref, q_ref, k_ref, v_ref):
    h1 = (h[...].astype(F32) + dot(ctx[...], wo[0]).astype(LOW).astype(F32)).astype(LOW)
    wide, scale = spread(h1)
    b = (wide * scale).astype(LOW)
    ff, size = wg.shape[2], 512
    acts = []
    for at in range(0, ff, size):
        gate, up, s = mlp_chunk(b, wg, wu, at, size)
        acts.append((gate * s * up).astype(LOW))
    down = dot(jnp.concatenate(acts, -1), wd[0])
    h2 = (wide + down.astype(LOW).astype(F32)).astype(LOW)
    out_ref[...] = h2
    queries_keys_values(h2, wq, wk, wv, cos, sin, q_ref, k_ref, v_ref)


def middle(ctx, h, wo, wg, wu, wd, wq, wk, wv, cos, sin, layer):
    t, d = h.shape
    n, ff = wq.shape[2], wg.shape[2]
    outs = [jax.ShapeDtypeStruct((t, d), LOW)] + [jax.ShapeDtypeStruct((t, n), LOW)] * 3
    return pl.pallas_call(
        middle_kernel,
        grid=(t // ROWS,),
        in_specs=[rows(n), rows(d)] + [matrix(w, layer) for w in (wo, wg, wu, wd)] + [matrix(w, layer + 1) for w in (wq, wk, wv)]
        + [rows(HEAD // 2)] * 2,
        out_specs=[rows(d)] + [rows(n)] * 3,
        out_shape=outs,
        compiler_params=params(30),
        cost_estimate=cost(2 * t * d * (4 * n + 3 * ff), h, h, *outs),
        name="middle",
    )(ctx, h, wo, wg, wu, wd, wq, wk, wv, cos, sin)


def causal_mask(size):
    return lax.broadcasted_iota(jnp.int32, (size, size), 1) >= lax.broadcasted_iota(jnp.int32, (size, size), 0)


def attention_kernel(q_ref, k_ref, v_ref, o_ref, lse_ref, mix_s, top_s):
    t, d = q_ref.shape
    e = d**-0.5 * LOG2E
    ones = jnp.ones((8, STRIP), LOW)
    blocks = [pl.ds(at, STRIP) for at in range(0, t, STRIP)]
    for j, keys in enumerate(blocks):
        k = k_ref[keys, :]
        values = jnp.concatenate([v_ref[keys, :].T, ones], axis=0)
        seen = blocks[j:]
        scores = [dot(k, q_ref[qs, :], 1, 1) for qs in seen]
        weights, keeps = [], []
        for qs, s in zip(seen, scores):
            if qs is keys:
                s = jnp.where(causal_mask(STRIP), s, HIDDEN)
            top = s.max(axis=0, keepdims=True)
            if j:
                old = top_s[0:1, qs]
                top = jnp.maximum(old, top)
                keeps.append(jnp.exp2((old - top) * e))
            top_s[0:1, qs] = top
            weights.append(jnp.exp2((s - top) * e).astype(LOW))
        for n, (qs, p) in enumerate(zip(seen, weights)):
            new = dot(values, p, 1, 0)
            if j:
                new = mix_s[:, qs] * keeps[n] + new
            if qs is keys:
                total = new[d : d + 1, :]
                o_ref[qs, :] = (new[:d, :] * (1 / total)).T.astype(LOW)
                lse_ref[0, :, qs] = top_s[0:1, qs] * e + jnp.log(total) * LOG2E
            else:
                mix_s[:, qs] = new


def head_specs(t, count):
    return [pl.BlockSpec((t, HEAD), lambda i: (0, i))] * count


def attention(q, k, v):
    t, n = q.shape
    outs = [jax.ShapeDtypeStruct((t, n), LOW), jax.ShapeDtypeStruct((n // HEAD, 1, t), F32)]
    return pl.pallas_call(
        attention_kernel,
        grid=(n // HEAD,),
        in_specs=head_specs(t, 3),
        out_specs=[*head_specs(t, 1), pl.BlockSpec((1, 1, t), lambda i: (i, 0, 0))],
        out_shape=outs,
        scratch_shapes=[pltpu.VMEM((HEAD + 8, t), F32), pltpu.VMEM((8, t), F32)],
        compiler_params=params(24),
        cost_estimate=cost(2.5 * t * t * n, q, k, v, *outs),
        name="attention",
    )(q, k, v)


def attention_back_kernel(q_ref, k_ref, v_ref, do_ref, o_ref, lse_ref, h, cos, sin, *rest, deeper):
    if deeper:
        by_h1, wq, wk, wv = rest[:4]
        by_h, grads, dq_s, at_s, by_q, by_k, by_v, mine, sem, by_a = rest[4:]
    else:
        late = rest[1]
        grads, dq_s, at_s, by_q, by_k, by_v, mine, sem = rest[-8:]
    t, d = q_ref.shape
    n, head = grads.shape[0], pl.program_id(0)
    scale = d**-0.5
    e = scale * LOG2E
    blocks = [pl.ds(at, STRIP) for at in range(0, t, STRIP)]

    @pl.when(head == 0)
    def _():
        for qs in blocks:
            wide, size = spread(h[qs, :])
            at_s[:, qs] = (wide * size).astype(LOW).T

    deltas = []
    for qs in blocks:
        both = do_ref[qs, :].astype(F32) * o_ref[qs, :].astype(F32)
        folded = sum(both[:, at : at + 128] for at in range(0, d, 128))
        deltas.append(folded.T.sum(axis=0, keepdims=True))
    for j, keys in enumerate(blocks):
        k, v = k_ref[keys, :], v_ref[keys, :]
        kt = k.T
        seen = list(enumerate(blocks))[j:]
        scores = [dot(k, q_ref[qs, :], 1, 1) for _, qs in seen]
        dps = [dot(v, do_ref[qs, :], 1, 1) for _, qs in seen]
        ps, dss = [], []
        for m, (x, qs) in enumerate(seen):
            p = jnp.exp2(scores[m] * e - lse_ref[0, :, qs])
            if x == j:
                p = jnp.where(causal_mask(STRIP), p, 0.0)
            ds = (p * (dps[m] - deltas[x])).astype(LOW)
            ps.append(p.astype(LOW))
            dss.append(ds)
            new = dot(kt, ds, 1, 0)
            if j:
                new = dq_s[:, qs] + new
            if x == j:
                by_q[qs, :] = turn((new * scale).T.astype(LOW), cos[qs, :], -sin[qs, :])
            else:
                dq_s[:, qs] = new
        late_q = pl.ds(j * STRIP, t - j * STRIP)
        by_v[keys, :] = dot(jnp.concatenate(ps, axis=1), do_ref[late_q, :], 1, 0).astype(LOW)
        dk = (dot(jnp.concatenate(dss, axis=1), q_ref[late_q, :], 1, 0) * scale).astype(LOW)
        by_k[keys, :] = turn(dk, cos[keys, :], -sin[keys, :])

    r = at_s.shape[0] // n
    for i, by in enumerate((by_q, by_k, by_v)):
        mine[:, i * r : (i + 1) * r, :] = dot(at_s[...], by[...]).reshape(n, r, d).astype(LOW)
    base = 0 if deeper else grads.shape[1] - 6 * r
    copies = [pltpu.make_async_copy(mine, grads.at[:, pl.ds(base, 3 * r), pl.ds(pl.multiple_of(head * d, d), d)], sem.at[0])]
    copies[0].start()
    if not deeper:
        copies.append(pltpu.make_async_copy(late, grads.at[:, pl.ds(base + 3 * r, 3 * r), :], sem.at[1]))

        @pl.when(head == 0)
        def _():
            copies[1].start()
            copies[1].wait()
    else:
        for qs in blocks:
            term = dot(by_q[qs, :], wq[0], 1, 1) + dot(by_k[qs, :], wk[0], 1, 1) + dot(by_v[qs, :], wv[0], 1, 1)
            by_a[qs, :] = jnp.where(head == 0, term, by_a[qs, :] + term)

        @pl.when(head == pl.num_programs(0) - 1)
        def _():
            for qs in blocks:
                wide, size = spread(h[qs, :])
                back = norm_back(wide, size, by_a[qs, :].astype(LOW).astype(F32)).astype(LOW).astype(F32)
                by_h[qs, :] = (by_h1[qs, :].astype(F32) + back).astype(LOW)
    copies[0].wait()


def attention_back(q, k, v, by, out, lse, h, cos, sin, n, layer, by_h1=None, wq=None, wk=None, wv=None, packed=None, late=None, after=()):
    t, width = q.shape
    d = h.shape[1]
    deeper = packed is None
    once = lambda a: pl.BlockSpec(a.shape, lambda i: (0,) * a.ndim, pipeline_mode=pl.Buffered(1))
    anywhere = pl.BlockSpec(memory_space=pl.ANY)
    given = [q, k, v, by, out, lse, h, cos, sin]
    specs = [*head_specs(t, 5), pl.BlockSpec((1, 1, t), lambda i: (i, 0, 0)), once(h), once(cos), once(sin)]
    scratch = [pltpu.VMEM((HEAD, t), F32), pltpu.VMEM((d, t), LOW)] + [pltpu.VMEM((t, HEAD), LOW)] * 3
    scratch += [pltpu.VMEM((n, 3 * d // n, HEAD), LOW), pltpu.SemaphoreType.DMA((2,))]
    if deeper:
        given += [by_h1, wq, wk, wv]
        specs += [once(by_h1)] + [pl.BlockSpec((1, d, HEAD), lambda i: (layer, 0, i))] * 3
        outs = [jax.ShapeDtypeStruct((t, d), LOW), jax.ShapeDtypeStruct((n, 3 * d // n, width), LOW)]
        out_specs = [once(h), anywhere]
        scratch += [pltpu.VMEM((t, d), F32)]
    else:
        given += [packed, late, *after]
        specs += [anywhere, once(late)] + [anywhere] * len(after)
        outs, out_specs = [jax.ShapeDtypeStruct(packed.shape, LOW)], [anywhere]
    return pl.pallas_call(
        functools.partial(attention_back_kernel, deeper=deeper),
        grid=(width // HEAD,),
        in_specs=specs,
        out_specs=out_specs,
        out_shape=outs,
        scratch_shapes=scratch,
        input_output_aliases={} if deeper else {9: 0},
        compiler_params=params(62),
        cost_estimate=cost(6.25 * t * t * width + 2 * t * d * width * (6 if deeper else 3), q, k, v, by, out, h, h),
        name="attention_back",
    )(*given)


def mlp_back_kernel(ctx, h, by, wo, wg_in, wu_in, wd_in, by_h1, by_ctx, grads, acc_o, acc_g, acc_u, acc_d, b_s, bt_s, dyt_s, by_b, stage, sems,
                    wg, wu, wd, fetched, *, layer):
    step = pl.program_id(0)

    def fetches(c):
        here = pl.ds(pl.multiple_of(c * CHUNK, CHUNK), CHUNK)
        return [pltpu.make_async_copy(wg_in.at[layer, :, here], wg.at[0, :, here], fetched.at[0, c]),
                pltpu.make_async_copy(wu_in.at[layer, :, here], wu.at[0, :, here], fetched.at[1, c]),
                pltpu.make_async_copy(wd_in.at[layer, here, :], wd.at[0, here, :], fetched.at[2, c])]

    @pl.when(step == 0)
    def _():
        for c in range(wg.shape[2] // CHUNK):
            for fetch in fetches(c):
                fetch.start()

    last = step == pl.num_programs(0) - 1
    n, d, ff = grads.shape[0], wg.shape[1], wg.shape[2]
    r, rd, chunks = d // n, ff // n, ff // CHUNK
    many = CHUNK // rd

    def put(acc, where, term):
        acc[where] = jnp.where(step == 0, term, acc[where] + term)

    def leave(owners, first, count, i, kind):
        where = (owners, pl.ds(first, count))
        return pltpu.make_async_copy(stage.at[where], grads.at[where], sems.at[kind, i])

    def leaving(c):
        gate_rows = pl.multiple_of(r + c * r, r)
        up_rows = pl.multiple_of(r + (chunks + c) * r, r)
        owners = pl.ds(pl.multiple_of(c * many, many), many)
        return gate_rows, up_rows, owners, (leave(pl.ds(0, n), gate_rows, r, c, 0), leave(pl.ds(0, n), up_rows, r, c, 1),
                                            leave(owners, r * (1 + 2 * chunks), rd, c, 2))

    h1 = (h[...].astype(F32) + dot(ctx[...], wo[0]).astype(LOW).astype(F32)).astype(LOW)
    wide, scale = spread(h1)
    b = (wide * scale).astype(LOW)
    b_s[...] = b
    bt_s[...] = b.T
    dyt_s[...] = by[...].T
    by_b[...] = jnp.zeros(by_b.shape, F32)

    def chunk(c):
        here = pl.ds(pl.multiple_of(c * CHUNK, CHUNK), CHUNK)
        gate, up = dot(b_s[...], wg[0, :, here]), dot(b_s[...], wu[0, :, here])
        s = 0.5 * jnp.tanh(0.5 * gate) + 0.5
        by_act = dot(by[...], wd[0, here, :], 1, 1).astype(LOW).astype(F32)
        silu = gate * s
        act = (silu * up).astype(LOW)
        by_up = (by_act * silu).astype(LOW)
        by_gate = (by_act * up * (s + silu * (1.0 - s))).astype(LOW)
        by_b[...] += dot(by_gate, wg[0, :, here], 1, 1) + dot(by_up, wu[0, :, here], 1, 1)
        put(acc_d, (slice(None), here), dot(dyt_s[...], act))
        put(acc_g, (slice(None), here), dot(bt_s[...], by_gate))
        put(acc_u, (slice(None), here), dot(bt_s[...], by_up))

    def two(i, _):
        @pl.when(step == 0)
        def _():
            for c in (2 * i, 2 * i + 1):
                for fetch in fetches(c):
                    fetch.wait()

        for c in (2 * i, 2 * i + 1):
            chunk(c)

        @pl.when(last)
        def _():
            for c in (2 * i, 2 * i + 1):
                here = pl.ds(pl.multiple_of(c * CHUNK, CHUNK), CHUNK)
                gate_rows, up_rows, owners, copies = leaving(c)
                stage[:, pl.ds(gate_rows, r), :] = acc_g[:, here].reshape(n, r, CHUNK).astype(LOW)
                stage[:, pl.ds(up_rows, r), :] = acc_u[:, here].reshape(n, r, CHUNK).astype(LOW)
                stage[owners, r * (1 + 2 * chunks) :, :] = acc_d[:, here].T.reshape(many, rd, d).astype(LOW)
                for copy in copies:
                    copy.start()

    lax.fori_loop(0, chunks // 2, two, None)
    wide, scale = spread(h1)
    total = (by[...].astype(F32) + norm_back(wide, scale, by_b[...].astype(LOW).astype(F32)).astype(LOW).astype(F32)).astype(LOW)
    by_h1[...] = total
    by_ctx[...] = dot(total, wo[0], 1, 1).astype(LOW)
    put(acc_o, (slice(None), slice(None)), dot(ctx[...].T, total))

    @pl.when(last)
    def _():
        stage[:, :r, :] = acc_o[...].reshape(n, r, d).astype(LOW)
        copy = leave(pl.ds(0, n), 0, r, 0, 3)
        copy.start()
        for c in range(chunks):
            for each in leaving(c)[3]:
                each.wait()
        copy.wait()


CHUNK = 512


def mlp_back(ctx, h, by, wo, wg, wu, wd, layer, n, room=0, size=512):
    t, d = h.shape
    heads, ff = wo.shape[1], wg.shape[2]
    packed = (heads * d + 3 * d * ff) // (512 * n)
    outs = [jax.ShapeDtypeStruct((t, d), LOW), jax.ShapeDtypeStruct((t, heads), LOW), jax.ShapeDtypeStruct((n, packed + room, 512), LOW)]
    return pl.pallas_call(
        functools.partial(mlp_back_kernel, layer=layer),
        grid=(t // size,),
        in_specs=[rows(heads, size), rows(d, size), rows(d, size), matrix(wo, layer)] + [pl.BlockSpec(memory_space=pl.ANY)] * 3,
        out_specs=[rows(d, size), rows(heads, size), pl.BlockSpec(memory_space=pl.ANY)],
        out_shape=outs,
        scratch_shapes=[pltpu.VMEM((heads, d), F32)] + [pltpu.VMEM((d, ff), F32)] * 3
        + [pltpu.VMEM((size, d), LOW), pltpu.VMEM((d, size), LOW), pltpu.VMEM((d, size), LOW), pltpu.VMEM((size, d), F32)]
        + [pltpu.VMEM((n, packed, 512), LOW), pltpu.SemaphoreType.DMA((4, ff // CHUNK))]
        + [pltpu.VMEM((1,) + w.shape[1:], LOW) for w in (wg, wu, wd)] + [pltpu.SemaphoreType.DMA((3, ff // CHUNK))],
        compiler_params=params(62),
        cost_estimate=cost(2 * t * d * (8 * ff + 3 * heads), h, h, h, *outs),
        name="mlp_back",
    )(ctx, h, by, wo, wg, wu, wd)


def layers_of(plan):
    return {i: [layer for j, layer in plan if j == i] for i in sorted({i for i, _ in plan})}


def adamw_kernel(me, packed_g, *refs, plan):
    used = layers_of(plan)
    count = len(used)
    ws, ms, vs = (dict(zip(used, refs[k * count : (k + 1) * count])) for k in range(3))
    rest = refs[-1 - 2 * count :]
    packed, new_m, new_v = rest[0], dict(zip(used, rest[1 : 1 + count])), dict(zip(used, rest[1 + count :]))
    at = 0
    for i, layer in plan:
        x = layer - used[i][0]
        r, width = ms[i].shape[1], ms[i].shape[2]
        for c in range(0, width, 512):
            cols = slice(c, c + 512)
            g = packed_g[at : at + r, :].astype(F32)
            m = 0.9 * ms[i][x, :, cols] + 0.1 * g
            v = 0.95 * vs[i][x, :, cols] + 0.05 * g * g
            w = ws[i][x, :, cols].astype(F32)
            new_m[i][x, :, cols] = m
            new_v[i][x, :, cols] = v
            packed[at : at + r, :] = (w - 0.02 * (m * lax.rsqrt(v + 1e-8) + 0.1 * w)).astype(LOW)
            at += r


def adamw(me, g, ws, ms, vs, plan, earlier=None, after=()):
    used, earlier = layers_of(plan), earlier or {}
    spec = lambda i, mine: pl.BlockSpec((len(used[i]),) + ms[i].shape[1:], lambda _, me: (used[i][0], me[0] if mine else 0, 0))
    own, part = [spec(i, True) for i in used], [spec(i, False) for i in used]
    total = g.shape[0]
    outs = [jax.ShapeDtypeStruct((total, 512), LOW)] + [jax.ShapeDtypeStruct(ms[i].shape, F32) for _ in range(2) for i in used]
    known = [earlier[i][k] for k in range(2) for i in earlier]
    given = [g] + [a[i] for a in (ws, ms, vs) for i in used] + known + list(after)
    first = 2 + 3 * len(used)
    to = [1 + k * len(used) + list(used).index(i) for k in range(2) for i in earlier]
    new, *moments = pl.pallas_call(
        functools.partial(adamw_kernel, plan=plan),
        grid_spec=pltpu.PrefetchScalarGridSpec(
            num_scalar_prefetch=1,
            grid=(1,),
            in_specs=[pl.BlockSpec(g.shape, lambda _, me: (0, 0)), *own, *part, *part] + [pl.BlockSpec(memory_space=pl.ANY)] * len([*known, *after]),
            out_specs=[pl.BlockSpec((total, 512), lambda _, me: (0, 0)), *part, *part],
        ),
        out_shape=outs,
        input_output_aliases={first + i: o for i, o in enumerate(to)},
        compiler_params=params(54 if earlier else 62),
        cost_estimate=cost(20 * total * 512, g, *outs),
        name="adamw",
    )(me, *given)
    return new, {i: (moments[x], moments[x + len(used)]) for x, i in enumerate(used)}


def unpack_kernel(packed, *refs, plan):
    used = layers_of(plan)
    outs, at = dict(zip(used, refs[-len(used) :])), 0
    owners = packed.shape[0]
    for i, layer in plan:
        out = outs[i]
        r = out.shape[1] // owners
        for c in range(0, out.shape[2], 512):
            for owner in range(owners):
                out[layer - used[i][0], owner * r : (owner + 1) * r, c : c + 512] = packed[owner, at : at + r, :]
            at += r


def unpack(packed, ws, n, plan, earlier=None):
    used, earlier = layers_of(plan), earlier or {}
    outs = [jax.ShapeDtypeStruct(ws[i].shape, LOW) for i in used]
    total = packed.shape[0] // n
    some = min(n, 4)
    new = pl.pallas_call(
        functools.partial(unpack_kernel, plan=plan),
        grid=(n // some,),
        in_specs=[pl.BlockSpec((some, total, 512), lambda i: (i, 0, 0))] + [pl.BlockSpec(memory_space=pl.ANY)] * len(earlier),
        out_specs=[pl.BlockSpec((len(used[i]), some * ws[i].shape[1] // n, ws[i].shape[2]), lambda at, i=i: (used[i][0], at, 0)) for i in used],
        out_shape=outs,
        input_output_aliases={1 + x: list(used).index(i) for x, i in enumerate(earlier)},
        compiler_params=params(62),
        cost_estimate=cost(0, *outs),
        name="unpack",
    )(packed.reshape(n, total, 512), *earlier.values())
    return dict(zip(used, new))


CORES = 2
PARTS = 4


def part_rows(total):
    long = -(-total // (2 * 16 * 2)) * 16
    short = total // 2 - long
    return (0, long), (long, short), (total // 2, long), (total // 2 + long, short)


def reduce_kernel(g, out, mine, pair, sent, got, mine_sem, pair_send, pair_got, send_sem, got_sem):
    n, total = g.shape[0], g.shape[1]
    chips = n // CORES
    far, parts = chips // 2, part_rows(total)
    me = lax.axis_index("dp")
    z, core = lax.div(me, CORES), lax.rem(me, CORES)
    at = lambda chip, which: {"dp": lax.rem(chip + chips, chips) * CORES + which}
    peers = {1: at(z + 1, core), -1: at(z - 1, core)}
    partner = at(z, 1 - core)

    barrier = pltpu.get_barrier_semaphore()
    for peer in (peers[1], peers[-1], partner):
        pl.semaphore_signal(barrier, inc=1, device_id=peer, device_id_type=pl.DeviceIdType.MESH)

    order = [far] + [x * sign for x in range(far - 1, 0, -1) for sign in (1, -1)] + [0]
    slot = {offset: i for i, offset in enumerate(order)} | {-far: 0}
    local = []
    for i, offset in enumerate(order):
        chunk = lax.rem(z + offset + chips, chips) * CORES
        local.append(pltpu.make_async_copy(g.at[chunk + core], mine.at[i], mine_sem.at[i]))
        local[i].start()
    pl.semaphore_wait(barrier, 3)
    across = []
    for i, offset in enumerate(order):
        chunk = lax.rem(z + offset + chips, chips) * CORES
        across.append(pltpu.make_async_remote_copy(g.at[chunk + 1 - core], pair.at[i], pair_send.at[i], pair_got.at[i], device_id=partner,
                                                   device_id_type=pl.DeviceIdType.MESH))
        across[i].start()

    streams = [(sign, part, far if (part < PARTS // 2) == (sign > 0) else far - 1) for part in range(PARTS) for sign in (1, -1)]
    ready, copies = set(), {}

    def own(offset, here):
        i = slot[offset]
        if i not in ready:
            ready.add(i)
            local[i].wait()
            across[i].wait_recv()
        return mine[i, here, :].astype(F32) + pair[i, here, :].astype(F32)

    for s in range(far):
        pending = None
        for x, (sign, part, hops) in enumerate(streams):
            if s < hops:
                value = own(sign * (hops - s), pl.ds(*parts[part]))
                if s:
                    copies[s - 1, x].wait_recv()
                    value = value + got[s - 1, x, : parts[part][1]].astype(F32)
                many = pl.ds(0, parts[part][1])
                sent[s, x, many] = value.astype(LOW)
                copies[s, x] = pltpu.make_async_remote_copy(sent.at[s, x, many], got.at[s, x, many], send_sem.at[s, x], got_sem.at[s, x],
                                                            device_id=peers[sign], device_id_type=pl.DeviceIdType.MESH)
                if pending is not None:
                    pending.start()
                pending = copies[s, x]
        pending.start()
    for part in range(PARTS):
        here = pl.ds(*parts[part])
        value = own(0, here)
        for x, (_, of, hops) in enumerate(streams):
            if of == part:
                copies[hops - 1, x].wait_recv()
                value = value + got[hops - 1, x, : parts[part][1]].astype(F32)
        out[here, :] = value.astype(LOW)
    for copy in (*across, *copies.values()):
        copy.wait_send()


def reduce(g):
    n, total, width = g.shape
    chips = n // CORES
    far, streams = chips // 2, 2 * PARTS
    out = jax.ShapeDtypeStruct((total, width), LOW)
    dma = lambda *shape: pltpu.SemaphoreType.DMA(shape)
    return pl.pallas_call(
        reduce_kernel,
        in_specs=[pl.BlockSpec(memory_space=pl.ANY)],
        out_specs=pl.BlockSpec(memory_space=pltpu.VMEM),
        out_shape=out,
        scratch_shapes=[pltpu.VMEM((chips, total, width), LOW)] * 2 + [pltpu.VMEM((far, streams, part_rows(total)[0][1], width), LOW)] * 2
        + [dma(chips)] * 3 + [dma(far, streams)] * 2,
        compiler_params=pltpu.CompilerParams(collective_id=1, has_side_effects=True, vmem_limit_bytes=55 * 2**20),
        cost_estimate=pl.CostEstimate(flops=50_000_000_000, transcendentals=0, bytes_accessed=g.size * 2),
        name="reduce",
    )(g)


def solution(mesh):
    n = mesh.shape["dp"]

    def scatter(g):
        return lax.psum_scatter(g.reshape(-1, g.shape[2]), "dp", scatter_dimension=0, tiled=True)

    def step(x, dy, *arrays):
        weights, m, v = (arrays[i : i + 7] for i in (0, 7, 14))
        wq, wk, wv, wo, wg, wu, wd = weights
        h0, t = x[0], x.shape[1]
        half = HEAD // 2
        rate = THETA ** (-jnp.arange(half, dtype=F32) / half)
        high = (jnp.arange(t // 64, dtype=F32) * 64)[:, None, None] * rate
        low = jnp.arange(64, dtype=F32)[:, None] * rate
        ch, sh, cl, sl = lax.optimization_barrier((jnp.cos(high), jnp.sin(high), jnp.cos(low), jnp.sin(low)))
        cos, sin = (ch * cl - sh * sl).reshape(t, half), (sh * cl + ch * sl).reshape(t, half)
        me = lax.axis_index("dp").astype(jnp.int32).reshape(1)
        q0, k0, v0 = first(h0, wq, wk, wv, cos, sin, 0)
        c0, l0 = attention(q0, k0, v0)
        h1, q1, k1, v1 = middle(c0, h0, wo, wg, wu, wd, wq, wk, wv, cos, sin, 0)
        c1, l1 = attention(q1, k1, v1)
        by, by_c, g1 = mlp_back(c1, h1, dy[0], wo, wg, wu, wd, 1, n)
        r1 = scatter(g1)
        by, late = attention_back(q1, k1, v1, by_c, c1, l1, h1, cos, sin, n, 1, by, wq, wk, wv)
        by, by_c, g0 = mlp_back(c0, h0, by, wo, wg, wu, wd, 0, n, 2 * late.shape[1])
        new1, moments = adamw(me, r1, weights, m, v, LATE, after=(by_c,))
        all1 = lax.all_gather(new1, "dp", axis=0, tiled=True)
        (g0,) = attention_back(q0, k0, v0, by_c, c0, l0, h0, cos, sin, n, 0, packed=g0, late=late, after=(new1,))
        new0, moments = adamw(me, reduce(g0), weights, m, v, EARLY, moments)
        all0 = lax.all_gather(new0, "dp", axis=0, tiled=True)
        new = unpack(all0, weights, n, EARLY, unpack(all1, weights, n, LATE))
        return tuple(new[i] for i in range(7)) + tuple(moments[i][which] for which in range(2) for i in range(7))

    states, all_of, cut = P(("rep", "dp"), None, None), P(None, None, None), P(None, "dp", None)
    return jax.shard_map(
        step,
        mesh=mesh,
        in_specs=(states, states) + (all_of,) * 7 + (cut,) * 14,
        out_specs=(P("rep", None, None),) * 7 + (P("rep", "dp", None),) * 14,
        check_vma=False,
    )
```
